32 devices in a mesh: grp: 4 (over y, x), dev: 8 (over z, core).
Axes of the slice: x: 2, y: 2, z: 4, core: 2. Of those that a mesh axis runs over, the one named last changes fastest.
Arguments:
- leaf_emit: float32 [3, 4096], P(None, 'dev'), may hold values from 0 to 1
- leaf_albedo: float32 [3, 4096], P(None, 'dev'), may hold values from 0.2 to 0.9
- leaf_radiosity: float32 [3, 4096], P(None, 'dev'), may hold values from 0.05 to 4
- leaf_area: float32 [4096], P('dev'), may hold values from 0.002 to 0.03
- parent_index: int32 [4096], P('dev'), may hold values from 0 to 255, as said below
- node_position: float32 [3, 6144], P(None, 'dev'), may hold values from -1 to 1
- node_angles: float32 [2, 6144], P(None, 'dev'), may hold values from -3.140625 to 3.140625
- block_receiver: int32 [4, 1024], P('grp', 'dev'), may hold values from 0 to 5
- block_source: int32 [4, 1024], P('grp', 'dev'), may hold values from 0 to 15
- block_count: int32 [4, 8], P('grp', 'dev'), may hold values from 16 to 128, as said below
Outputs:
- new_radiosity: float32 [3, 4096], P(None, 'dev')
The draws below stay inside these ranges and needn't reach their ends.
Inputs may be any that keep to these rules, and one draw needn't show every extreme that they name: `parent_index`: within each shard's 512 leaves every cluster 0 to 255 is named at least once. The first block_count slots of a device are live, the rest are ignored. For every index of dev exactly one index of grp has 128 live slots; the others have at most 64.
All inputs are finite; a program needn't handle non-finite values.
Results may differ from the reference program's by a relative error of at most 0.0001.
Values sent between devices are 32-bit elements; how exact they have to be, the bound alone decides.
A program may use at most 64 MiB of HBM per device.

```python
import math
import jax
import jax.numpy as jnp
from jax import lax

TILE = 128
LEAF_DEV = 512
PAR_DEV = 256
BLK = 128
GROUPS = 4
SHARDS = 8
NODE_DEV = 768
NT = 6
SRC_TILES = 16
LEAVES = 4096
NODES = 6144


def draw_parent_index(key, part):
    shard_count = LEAVES // LEAF_DEV
    shard_keys = jax.random.split(key, shard_count)

    def one_shard(shard_key):
        first_key, second_key = jax.random.split(shard_key)
        covered = jnp.arange(PAR_DEV, dtype=jnp.int32)
        others = jax.random.randint(first_key, (LEAF_DEV - PAR_DEV,), 0, PAR_DEV, dtype=jnp.int32)
        return jax.random.permutation(second_key, jnp.concatenate([covered, others]))
    return jax.vmap(one_shard)(shard_keys).reshape(LEAVES).astype(jnp.int32)


def draw_block_count(key, part):
    first_key, second_key = jax.random.split(jax.random.fold_in(key, 7))
    counts = jax.random.randint(first_key, (GROUPS, SHARDS), BLK // 8, BLK // 2 + 1, dtype=jnp.int32)
    heavy = jax.random.randint(second_key, (SHARDS,), 0, GROUPS, dtype=jnp.int32)
    group_rows = jnp.arange(GROUPS, dtype=jnp.int32)[:, None]
    return jnp.where(group_rows == heavy[None, :], BLK, counts).astype(jnp.int32)


def set_ends(entries, rng, least, high):
    longest = entries.shape.index(max(entries.shape))
    spots = []
    for shift in (0, 1):
        where = [jax.random.randint(jax.random.fold_in(rng, axis), (), 0, length) for axis, length in enumerate(entries.shape)]
        where[longest] = (where[longest] + shift) % entries.shape[longest]
        spots.append(tuple(where))
    return entries.at[spots[0]].set(least).at[spots[1]].set(high)


def steps_of(stream_key, extent, pieces, low, high):
    factor_of, own = 1.0, jax.random.fold_in(stream_key, 6)
    for position, shards_of in pieces:
        draws = jnp.exp(jax.random.uniform(jax.random.fold_in(own, position), (shards_of,), jnp.float32, low / len(pieces), high / len(pieces)))
        factor_of = factor_of * jnp.repeat(draws, extent[position] // shards_of).reshape([-1 if axis == position else 1 for axis in range(len(extent))])
    return factor_of


def setup_inputs(seed: int = 0) -> dict:
    key_list = jax.random.split(jax.random.key(seed), 11)
    leaf_emit = jnp.clip(1.0 * jax.random.uniform(key_list[0], (3, LEAVES), jnp.float32) ** steps_of(key_list[0], (3, LEAVES), ((1, 8),), -0.2, 0.2), 0.0, 1.0)
    leaf_albedo = jnp.clip(0.2 + 0.7 * jax.random.uniform(key_list[1], (3, LEAVES), jnp.float32) ** steps_of(key_list[1], (3, LEAVES), ((1, 8),), -0.2, 0.2), 0.2, 0.9)
    leaf_radiosity = jnp.clip(jnp.exp(math.log(4.0) - 4.3820266 * jax.random.uniform(key_list[2], (3, LEAVES), jnp.float32) ** steps_of(key_list[2], (3, LEAVES), ((1, 8),), -0.2, 0.2)), 0.05, 4.0)
    leaf_area = jnp.clip(jnp.exp(math.log(0.03) - 2.70805 * jax.random.uniform(key_list[3], (LEAVES,), jnp.float32) ** steps_of(key_list[3], (LEAVES,), ((0, 8),), -0.2, 0.2)), 0.002, 0.03)
    parent_index = draw_parent_index(jax.random.fold_in(key_list[10], 71), 0)
    node_position = jnp.clip(jax.random.uniform(key_list[5], (3, NODES), jnp.float32, -1.0, 1.0) * steps_of(key_list[5], (3, NODES), ((1, 8),), -0.4, 0.0), -1.0, 1.0)
    node_angles = jnp.clip(jax.random.uniform(key_list[6], (2, NODES), jnp.float32, -3.140625, 3.140625), -3.140625, 3.140625)
    block_receiver = set_ends(jax.random.randint(key_list[7], (GROUPS, SHARDS * BLK), 0, NT), jax.random.fold_in(key_list[7], 1), 0, NT - 1).astype(jnp.int32)
    block_source = set_ends(jax.random.randint(key_list[8], (GROUPS, SHARDS * BLK), 0, SRC_TILES), jax.random.fold_in(key_list[8], 1), 0, SRC_TILES - 1).astype(jnp.int32)
    block_count = draw_block_count(jax.random.fold_in(key_list[10], 71), 0)
    return {"leaf_emit": leaf_emit, "leaf_albedo": leaf_albedo, "leaf_radiosity": leaf_radiosity, "leaf_area": leaf_area, "parent_index": parent_index, "node_position": node_position, "node_angles": node_angles, "block_receiver": block_receiver, "block_source": block_source, "block_count": block_count}


def unit_normals(node_angles):
    azimuth = node_angles[0]
    elevation = node_angles[1]
    return jnp.stack([jnp.cos(azimuth) * jnp.cos(elevation), jnp.sin(azimuth) * jnp.cos(elevation), jnp.sin(elevation)])


def tile_irradiance(receivers, sources):
    offsets = [sources[axis_id][:, None, :] - receivers[axis_id][:, :, None] for axis_id in range(3)]
    distance_sq = offsets[0] * offsets[0] + offsets[1] * offsets[1] + offsets[2] * offsets[2]
    facing_receiver = receivers[3][:, :, None] * offsets[0] + receivers[4][:, :, None] * offsets[1] + receivers[5][:, :, None] * offsets[2]
    facing_source = sources[3][:, None, :] * offsets[0] + sources[4][:, None, :] * offsets[1] + sources[5][:, None, :] * offsets[2]
    source_area = sources[6][:, None, :]
    factor = source_area * jnp.maximum(facing_receiver, 0.0) * jnp.maximum(-facing_source, 0.0) / ((distance_sq + source_area) * (jnp.pi * distance_sq + source_area))
    return jnp.einsum('bij,cbj->bci', factor, sources[7:10], precision=lax.Precision.HIGHEST)


def reference(leaf_emit, leaf_albedo, leaf_radiosity, leaf_area, parent_index, node_position, node_angles, block_receiver, block_source, block_count):
    shard_count = SHARDS
    per_peer = NODE_DEV // shard_count
    normals = unit_normals(node_angles)
    positions = node_position.reshape(3, shard_count, NODE_DEV)
    normals = normals.reshape(3, shard_count, NODE_DEV)
    patch_area = leaf_area.reshape(shard_count, LEAF_DEV)
    radiosity = leaf_radiosity.reshape(3, shard_count, LEAF_DEV)
    parents = parent_index.reshape(shard_count, LEAF_DEV)
    parent_onehot = (parents[:, :, None] == jnp.arange(PAR_DEV, dtype=jnp.int32)[None, None, :]).astype(jnp.float32)
    cluster_area = jnp.einsum('sl,slp->sp', patch_area, parent_onehot, precision=lax.Precision.HIGHEST)
    weighted = jnp.einsum('csl,slp->csp', radiosity * patch_area[None], parent_onehot, precision=lax.Precision.HIGHEST)
    cluster_radiosity = weighted / cluster_area[None]
    source_pack = jnp.concatenate([positions[:, :, LEAF_DEV:], normals[:, :, LEAF_DEV:], cluster_area[None], cluster_radiosity], axis=0)
    source_tiles = source_pack.reshape(10, SRC_TILES, TILE)
    receiver_octree = jnp.concatenate([positions, normals], axis=0)
    receiver_link = receiver_octree.reshape(6, shard_count, shard_count, per_peer).transpose(0, 2, 1, 3)
    receiver_tiles = receiver_link.reshape(6, shard_count * NT, TILE)
    tile_offset = (jnp.arange(shard_count, dtype=jnp.int32) * NT)[None, :, None]
    receiver_ids = (block_receiver.reshape(GROUPS, shard_count, BLK) + tile_offset).reshape(GROUPS * shard_count, BLK)
    source_ids = block_source.reshape(GROUPS * shard_count, BLK)
    live_weight = (jnp.arange(BLK, dtype=jnp.int32)[None, None, :] < block_count[:, :, None]).astype(jnp.float32)
    live_weight = live_weight.reshape(GROUPS * shard_count, BLK)

    def accumulate(totals, batch):
        batch_receivers, batch_sources, batch_weight = batch
        receivers = jnp.take(receiver_tiles, batch_receivers, axis=1)
        sources = jnp.take(source_tiles, batch_sources, axis=1)
        contrib = tile_irradiance(receivers, sources) * batch_weight[:, None, None]
        return totals.at[batch_receivers].add(contrib), None

    initial = jnp.zeros((shard_count * NT, 3, TILE), jnp.float32)
    totals, unused = lax.scan(accumulate, initial, (receiver_ids, source_ids, live_weight))
    link_order = totals.reshape(shard_count, NT, 3, TILE).transpose(2, 0, 1, 3).reshape(3, shard_count, NODE_DEV)
    octree_order = link_order.reshape(3, shard_count, shard_count, per_peer).transpose(0, 2, 1, 3).reshape(3, shard_count, NODE_DEV)
    pushed = jnp.einsum('csp,slp->csl', octree_order[:, :, LEAF_DEV:], parent_onehot, precision=lax.Precision.HIGHEST)
    gathered = octree_order[:, :, :LEAF_DEV] + pushed
    return leaf_emit + leaf_albedo * gathered.reshape(3, shard_count * LEAF_DEV)
```

```python
import functools
import jax
import jax.numpy as jnp
from jax import lax
from jax.experimental import pallas as pl
from jax.experimental.pallas import tpu as pltpu
from jax.sharding import PartitionSpec as P

TILE = 128


batch_slots = 16


def unit_normals(node_angles):
    azimuth = node_angles[0]
    elevation = node_angles[1]
    return jnp.stack(
        [
            jnp.cos(azimuth) * jnp.cos(elevation),
            jnp.sin(azimuth) * jnp.cos(elevation),
            jnp.sin(elevation),
        ]
    )


def tile_irradiance(receivers, sources):
    offsets = [
        sources[axis_id][:, None, :] - receivers[axis_id][:, :, None] for axis_id in range(3)
    ]
    distance_sq = offsets[0] * offsets[0] + offsets[1] * offsets[1] + offsets[2] * offsets[2]
    facing_receiver = (
        receivers[3][:, :, None] * offsets[0]
        + receivers[4][:, :, None] * offsets[1]
        + receivers[5][:, :, None] * offsets[2]
    )
    facing_source = (
        sources[3][:, None, :] * offsets[0]
        + sources[4][:, None, :] * offsets[1]
        + sources[5][:, None, :] * offsets[2]
    )
    source_area = sources[6][:, None, :]
    factor = (
        source_area
        * jnp.maximum(facing_receiver, 0.0)
        * jnp.maximum(-facing_source, 0.0)
        / ((distance_sq + source_area) * (jnp.pi * distance_sq + source_area))
    )
    return jnp.einsum("bij,cbj->bci", factor, sources[7:10], precision=lax.Precision.HIGHEST)


def listed_body(
    leaf_emit,
    leaf_albedo,
    leaf_radiosity,
    leaf_area,
    parent_index,
    node_position,
    node_angles,
    block_receiver,
    block_source,
    block_count,
):
    leaf_count = leaf_area.shape[0]
    node_count = node_position.shape[1]
    cluster_count = node_count - leaf_count
    tile_count = node_count // TILE
    slot_count = block_receiver.shape[1]
    normals = unit_normals(node_angles)
    parent_onehot = (
        parent_index[:, None] == jnp.arange(cluster_count, dtype=jnp.int32)[None, :]
    ).astype(jnp.float32)
    cluster_area = jnp.dot(leaf_area, parent_onehot, precision=lax.Precision.HIGHEST)
    weighted = jnp.dot(
        leaf_radiosity * leaf_area[None, :], parent_onehot, precision=lax.Precision.HIGHEST
    )
    cluster_radiosity = weighted / cluster_area[None, :]
    source_pack = jnp.concatenate(
        [
            node_position[:, leaf_count:],
            normals[:, leaf_count:],
            cluster_area[None, :],
            cluster_radiosity,
        ],
        axis=0,
    )
    receiver_pack = jnp.concatenate([node_position, normals], axis=0)
    linked = lax.all_to_all(receiver_pack, "dev", split_axis=1, concat_axis=1, tiled=True)
    receiver_tiles = linked.reshape(6, tile_count, TILE)
    everything = lax.all_gather(source_pack, "dev", axis=1, tiled=True)
    source_tiles = everything.reshape(10, -1, TILE)
    receiver_ids = block_receiver[0]
    source_ids = block_source[0]
    live_count = block_count[0, 0]
    step_slots = min(batch_slots, slot_count)

    def add_batch(rounds, totals):
        first = rounds * step_slots
        batch_receivers = lax.dynamic_slice_in_dim(receiver_ids, first, step_slots, 0)
        batch_sources = lax.dynamic_slice_in_dim(source_ids, first, step_slots, 0)
        batch_weight = (first + jnp.arange(step_slots, dtype=jnp.int32) < live_count).astype(
            jnp.float32
        )
        receivers = jnp.take(receiver_tiles, batch_receivers, axis=1)
        sources = jnp.take(source_tiles, batch_sources, axis=1)
        contrib = tile_irradiance(receivers, sources) * batch_weight[:, None, None]
        placement = (
            batch_receivers[:, None] == jnp.arange(tile_count, dtype=jnp.int32)[None, :]
        ).astype(jnp.float32)
        return totals + jnp.einsum(
            "bt,bci->cti", placement, contrib, precision=lax.Precision.HIGHEST
        )

    batch_total = (live_count + step_slots - 1) // step_slots
    totals = lax.fori_loop(0, batch_total, add_batch, jnp.zeros((3, tile_count, TILE), jnp.float32))
    partial_value = totals.reshape(3, node_count)
    summed = lax.psum(partial_value, "grp")
    irradiance = lax.all_to_all(summed, "dev", split_axis=1, concat_axis=1, tiled=True)
    pushed = jnp.dot(irradiance[:, leaf_count:], parent_onehot.T, precision=lax.Precision.HIGHEST)
    gathered = irradiance[:, :leaf_count] + pushed
    return leaf_emit + leaf_albedo * gathered


F32 = jnp.float32
BF16 = jnp.bfloat16
MESH = pl.DeviceIdType.MESH
NT_DIMS = (((1,), (1,)), ((), ()))
FEATURES = 8
ROWS = 64


def split3(values):
    high = values.astype(BF16).astype(F32)
    rest = values - high
    middle = rest.astype(BF16).astype(F32)
    return high, middle, rest - middle


def stack3(values):
    rows = values.shape[0]
    pad = jnp.zeros((16 - 3 * rows, values.shape[1]), F32)
    return jnp.concatenate(list(split3(values)) + [pad], axis=0).astype(BF16)


def unstack3(product, rows):
    return product[0:rows] + product[rows : 2 * rows] + product[2 * rows : 3 * rows]


def flip(k, turn, shards):
    value, bit = 0, 1
    while bit < shards:
        digit = k // bit % 2
        value = value + bit * ((1 - digit) if turn // bit % 2 else digit)
        bit *= 2
    return value


def paired_rows(left, const):
    one, two, three = split3(left)
    row = lax.broadcasted_iota(jnp.int32, left.shape, 0)
    free = (row == 6) | (row == 7)
    plain = [jnp.where(free, 0.0, part) for part in (one, two, three)]
    zero = jnp.zeros_like(left)
    c1, c2, c3 = [zero] * 3 if const is None else split3(jnp.broadcast_to(const, left.shape))
    at6 = row == 6
    with_sum = jnp.where(free, left, one)
    return jnp.concatenate(
        [
            with_sum,
            jnp.where(at6, c1, plain[1]),
            jnp.where(at6, c2, plain[2]),
            with_sum,
            jnp.where(at6, c3, plain[1]),
            with_sum,
        ],
        axis=0,
    ).astype(BF16)


def dense_kernel(groups, shards, *refs):
    operands, count, out, inputs, scratch = refs[:7], refs[7], refs[8], refs[9:16], refs[16:]
    receiver_id, source_id, radiosity, area, parent, position, angles = inputs
    (
        load,
        sources, my_pack, my_hist, hists, right, onehot, place, columns, turned, sums,
        src_send, src_recv, hist_send, hist_recv,
    ) = scratch
    g = lax.axis_index("grp")
    k = lax.axis_index("dev")
    device_total = groups * shards
    me = g * shards + k
    leaves = radiosity.shape[1]
    nodes = position.shape[1]
    clusters = nodes - leaves
    per_shard = clusters // TILE
    source_tiles = shards * per_shard
    per_peer = nodes // shards
    chunks = nodes // TILE
    pairs = nodes // (2 * TILE)

    loads = [
        pltpu.make_async_copy(operands[i], inputs[i], load.at[i]) for i in range(len(inputs))
    ]
    for copy in loads:
        copy.start()

    barrier = pltpu.get_barrier_semaphore()
    far_first = sorted(range(shards), key=lambda step: -step)
    others = [
        ((g + group_step) % groups, flip(k, step, shards))
        for step in far_first
        for group_step in reversed(range(groups))
        if group_step or step
    ]
    for other in others:
        pl.semaphore_signal(barrier, inc=1, device_id=other, device_id_type=MESH)

    for copy in loads:
        copy.wait()

    lane = lax.broadcasted_iota(jnp.int32, (1, TILE), 1)
    code = jnp.where(
        lane < count[0, 0], receiver_id[...] * source_tiles + source_id[...], -1
    )
    square = lax.broadcasted_iota(jnp.int32, (TILE, TILE), 0)
    hit = jnp.where(square == code, 1.0, 0.0).astype(BF16)
    counted = lax.dot_general(
        jnp.ones((16, TILE), BF16), hit, NT_DIMS, preferred_element_type=F32
    )
    my_hist[...] = counted[0:1]
    hists[me] = counted[0:1]

    ids = lax.broadcasted_iota(jnp.int32, (clusters, leaves), 0)
    onehot[...] = jnp.where(ids == parent[...], 1.0, 0.0).astype(BF16)
    area_row = area[...]
    stacked = stack3(jnp.concatenate([area_row, radiosity[...] * area_row], axis=0))
    cluster = unstack3(
        lax.dot_general(stacked, onehot[...], NT_DIMS, preferred_element_type=F32), 4
    )
    cosines = jnp.cos(angles[...])
    sines = jnp.sin(angles[...])
    normals = jnp.concatenate(
        [cosines[0:1] * cosines[1:2], sines[0:1] * cosines[1:2], sines[1:2]], axis=0
    )
    first_band = cluster[1:2] * (1.0 / jnp.pi)
    facing = normals[:, leaves:] * first_band
    ratios = cluster[2:4] / cluster[1:2]
    for half in range(per_shard):
        here = slice(half * TILE, (half + 1) * TILE)
        there = slice(leaves + half * TILE, leaves + (half + 1) * TILE)
        my_pack[8 * half : 8 * half + 8, :] = jnp.concatenate(
            [position[:, there], facing[:, here], cluster[0:1, here], ratios[0:1, here]], axis=0
        )
        my_pack[8 * per_shard + half : 8 * per_shard + half + 1, :] = ratios[1:2, here]

    pl.semaphore_wait(barrier, device_total - 1)

    for other in others:
        pltpu.make_async_remote_copy(
            src_ref=my_hist,
            dst_ref=hists.at[me],
            send_sem=hist_send,
            recv_sem=hist_recv,
            device_id=other,
            device_id_type=MESH,
        ).start()

    def source_copy(step):
        return pltpu.make_async_remote_copy(
            src_ref=my_pack,
            dst_ref=sources.at[k],
            send_sem=src_send.at[step - 1],
            recv_sem=src_recv.at[k],
            device_id=(g, flip(k, step, shards)),
            device_id_type=MESH,
        )

    for step in far_first:
        if step:
            source_copy(step).start()

    middle = jnp.sum(position[...], axis=1, keepdims=True) * (1.0 / nodes)
    centred = position[...] - middle
    ones = jnp.ones((1, nodes), F32)
    none = jnp.zeros((1, nodes), F32)
    three = jnp.zeros((3, nodes), F32)
    offset = -jnp.sum(normals * centred, axis=0, keepdims=True)
    norm = jnp.sum(centred * centred, axis=0, keepdims=True)
    for which, rows in enumerate(
        (
            paired_rows(jnp.concatenate([normals, three, none, none], axis=0), offset),
            paired_rows(jnp.concatenate([three, centred, -ones, none], axis=0), None),
            paired_rows(jnp.concatenate([-2.0 * centred, three, none, ones], axis=0), norm),
        )
    ):
        right[which] = rows

    node = lax.broadcasted_iota(jnp.int32, (1, nodes), 1)
    link = jnp.zeros((1, nodes), jnp.int32)
    for j in range(1, shards):
        link += jnp.where(node >= j * per_peer, 1, 0)
    spot = k * per_peer + node - link * per_peer
    low_tile = k * per_peer // TILE
    high_tile = (k * per_peer + per_peer - 1) // TILE
    upper = spot >= (low_tile + 1) * TILE
    owner_row = lax.broadcasted_iota(jnp.int32, (device_total, nodes), 0) % shards
    hits = owner_row == link
    place[0] = jnp.where(hits & ~upper, 1.0, 0.0).astype(BF16)
    place[1] = jnp.where(hits & upper, 1.0, 0.0).astype(BF16)

    row8 = lax.broadcasted_iota(jnp.int32, (8, TILE), 0)
    centre8 = jnp.concatenate([middle, jnp.zeros((5, 1), F32)], axis=0)

    def tile_sums(pack, half, tile):
        values = pack[8 * half : 8 * half + 8, :]
        ratio = pack[8 * per_shard + half : 8 * per_shard + half + 1, :]
        area_here = values[6:7]
        shifted = values - centre8
        spots, aims = shifted[0:3], shifted[3:6]
        along = jnp.sum(spots * aims, axis=0, keepdims=True)
        reach = jnp.sum(spots * spots, axis=0, keepdims=True) + area_here
        one, two, low = split3(jnp.concatenate([spots, aims, along, reach], axis=0))
        left = jnp.concatenate(
            [
                one,
                jnp.where(row8 == 6, 1.0, one),
                jnp.where(row8 == 6, 1.0, one),
                two,
                jnp.where(row8 == 6, 1.0, two),
                low,
            ],
            axis=0,
        )
        extra = jnp.concatenate(
            [values[7:8], ratio, area_here * ((jnp.pi - 1.0) / jnp.pi), jnp.zeros((5, TILE), F32)],
            axis=0,
        )
        features = jnp.transpose(left).astype(BF16)
        column = jnp.transpose(extra)
        second, third, less = [
            jnp.broadcast_to(column[:, i : i + 1], (TILE, TILE)) for i in range(3)
        ]
        for pair in range(pairs):
            wide = slice(pair * 2 * TILE, (pair + 1) * 2 * TILE)
            totals = [[None] * 3, [None] * 3]
            for first in range(0, TILE, ROWS):
                some = slice(first, first + ROWS)
                toward, facing, span = [
                    jnp.dot(features[some], right[which, :, wide], preferred_element_type=F32)
                    for which in range(3)
                ]
                for side in range(2):
                    lanes = slice(side * TILE, (side + 1) * TILE)
                    u = span[:, lanes]
                    form = (
                        jnp.maximum(toward[:, lanes], 0.0)
                        * jnp.maximum(facing[:, lanes], 0.0)
                        / (u * (u - less[some]))
                    )
                    for c, scaled in enumerate((form, form * second[some], form * third[some])):
                        part = jnp.sum(scaled.reshape(ROWS // 8, 8, TILE), axis=0)
                        old = totals[side][c]
                        totals[side][c] = part if old is None else old + part
            for side in range(2):
                first = pair * 2 * TILE + side * TILE
                for c in range(3):
                    sums[tile, c : c + 1, first : first + TILE] = jnp.sum(
                        totals[side][c], axis=0, keepdims=True
                    )

    for first in range(0, shards, 2):
        packs = []
        for turn in (first, first + 1):
            owner = flip(k, turn, shards)
            if turn:
                pltpu.make_async_remote_copy(
                    src_ref=my_pack,
                    dst_ref=sources.at[owner],
                    send_sem=src_send.at[0],
                    recv_sem=src_recv.at[owner],
                    device_id=(g, owner),
                    device_id_type=MESH,
                ).wait_recv()
            packs.append((sources.at[owner] if turn else my_pack, owner))
        for pack, owner in packs:
            for half in range(per_shard):
                tile_sums(pack, half, owner * per_shard + half)

    all_but_one = hists.at[pl.ds(0, device_total - 1)]
    pltpu.make_async_copy(all_but_one, all_but_one, hist_recv).wait()
    table = jnp.concatenate([hists[d] for d in range(device_total)], axis=0)
    turned[...] = jnp.transpose(table)
    weight = jnp.zeros((source_tiles, nodes), F32)
    for which, tile in enumerate((low_tile, high_tile)):
        rows = turned[pl.ds(pl.multiple_of(tile * source_tiles, 8), source_tiles), :]
        weight += jnp.dot(rows.astype(BF16), place[which], preferred_element_type=F32)

    irradiance = weight[0:1] * sums[0]
    for tile in range(1, source_tiles):
        irradiance += weight[tile : tile + 1] * sums[tile]
    pushed = unstack3(
        jnp.dot(stack3(irradiance[:, leaves:]), onehot[...], preferred_element_type=F32), 3
    )
    out[...] = irradiance[:, :leaves] + pushed

    pltpu.make_async_copy(all_but_one, all_but_one, hist_send).wait()
    for step in far_first:
        if step:
            source_copy(step).wait_send()


def dense_body(
    groups, shards, leaf_emit, leaf_albedo, leaf_radiosity, leaf_area, parent_index,
    node_position, node_angles, block_receiver, block_source, block_count,
):
    leaves = leaf_area.shape[0]
    nodes = node_position.shape[1]
    clusters = nodes - leaves
    per_shard = clusters // TILE
    source_tiles = shards * per_shard
    device_total = groups * shards
    operands = (
        block_receiver, block_source, leaf_radiosity, leaf_area[None, :], parent_index[None, :],
        node_position, node_angles,
    )
    pack_rows = 9 * per_shard
    gathered = pl.pallas_call(
        functools.partial(dense_kernel, groups, shards),
        out_shape=pltpu.VMEM((3, leaves), F32),
        in_specs=[pl.BlockSpec(memory_space=pltpu.HBM)] * len(operands)
        + [pl.BlockSpec(memory_space=pltpu.SMEM)],
        out_specs=pl.BlockSpec(memory_space=pltpu.VMEM),
        scratch_shapes=[pltpu.VMEM(x.shape, x.dtype) for x in operands]
        + [
            pltpu.SemaphoreType.DMA((len(operands),)),
            pltpu.VMEM((shards, pack_rows, TILE), F32),
            pltpu.VMEM((pack_rows, TILE), F32),
            pltpu.VMEM((1, TILE), F32),
            pltpu.VMEM((device_total, 1, TILE), F32),
            pltpu.VMEM((3, 6 * FEATURES, nodes), BF16),
            pltpu.VMEM((clusters, leaves), BF16),
            pltpu.VMEM((2, device_total, nodes), BF16),
            pltpu.VMEM((TILE, TILE), F32),
            pltpu.VMEM((TILE, device_total), F32),
            pltpu.VMEM((source_tiles, 3, nodes), F32),
            pltpu.SemaphoreType.DMA((shards - 1,)),
            pltpu.SemaphoreType.DMA((shards,)),
            pltpu.SemaphoreType.DMA,
            pltpu.SemaphoreType.DMA,
        ],
        compiler_params=pltpu.CompilerParams(collective_id=0, has_side_effects=True),
    )(*operands, block_count)
    return leaf_emit + leaf_albedo * gathered


def body(groups, shards, *args):
    leaves, nodes, slots = args[3].shape[0], args[5].shape[1], args[7].shape[1]
    per_shard = (nodes - leaves) // TILE
    source_tiles = shards * per_shard
    dense = (
        nodes // TILE * source_tiles <= TILE
        and TILE % source_tiles == 0
        and source_tiles % 8 == 0
        and nodes % (2 * TILE) == 0
        and nodes % shards == 0
        and nodes // shards <= TILE
        and shards & (shards - 1) == 0
        and shards % 2 == 0
        and groups * shards <= TILE
        and slots == TILE
    )
    return dense_body(groups, shards, *args) if dense else listed_body(*args)


def solution(mesh):
    in_specs = (
        P(None, "dev"),
        P(None, "dev"),
        P(None, "dev"),
        P("dev"),
        P("dev"),
        P(None, "dev"),
        P(None, "dev"),
        P("grp", "dev"),
        P("grp", "dev"),
        P("grp", "dev"),
    )
    out_specs = P(None, "dev")
    sized = functools.partial(body, mesh.shape["grp"], mesh.shape["dev"])
    return jax.shard_map(sized, mesh=mesh, in_specs=in_specs, out_specs=out_specs, check_vma=False)
```

```python
import functools
import jax
import jax.numpy as jnp
from jax import lax
from jax.experimental import pallas as pl
from jax.experimental.pallas import tpu as pltpu
from jax.sharding import PartitionSpec as P

TILE = 128


batch_slots = 16


def unit_normals(node_angles):
    azimuth = node_angles[0]
    elevation = node_angles[1]
    return jnp.stack(
        [
            jnp.cos(azimuth) * jnp.cos(elevation),
            jnp.sin(azimuth) * jnp.cos(elevation),
            jnp.sin(elevation),
        ]
    )


def tile_irradiance(receivers, sources):
    offsets = [
        sources[axis_id][:, None, :] - receivers[axis_id][:, :, None] for axis_id in range(3)
    ]
    distance_sq = offsets[0] * offsets[0] + offsets[1] * offsets[1] + offsets[2] * offsets[2]
    facing_receiver = (
        receivers[3][:, :, None] * offsets[0]
        + receivers[4][:, :, None] * offsets[1]
        + receivers[5][:, :, None] * offsets[2]
    )
    facing_source = (
        sources[3][:, None, :] * offsets[0]
        + sources[4][:, None, :] * offsets[1]
        + sources[5][:, None, :] * offsets[2]
    )
    source_area = sources[6][:, None, :]
    factor = (
        source_area
        * jnp.maximum(facing_receiver, 0.0)
        * jnp.maximum(-facing_source, 0.0)
        / ((distance_sq + source_area) * (jnp.pi * distance_sq + source_area))
    )
    return jnp.einsum("bij,cbj->bci", factor, sources[7:10], precision=lax.Precision.HIGHEST)


def listed_body(
    leaf_emit,
    leaf_albedo,
    leaf_radiosity,
    leaf_area,
    parent_index,
    node_position,
    node_angles,
    block_receiver,
    block_source,
    block_count,
):
    leaf_count = leaf_area.shape[0]
    node_count = node_position.shape[1]
    cluster_count = node_count - leaf_count
    tile_count = node_count // TILE
    slot_count = block_receiver.shape[1]
    normals = unit_normals(node_angles)
    parent_onehot = (
        parent_index[:, None] == jnp.arange(cluster_count, dtype=jnp.int32)[None, :]
    ).astype(jnp.float32)
    cluster_area = jnp.dot(leaf_area, parent_onehot, precision=lax.Precision.HIGHEST)
    weighted = jnp.dot(
        leaf_radiosity * leaf_area[None, :], parent_onehot, precision=lax.Precision.HIGHEST
    )
    cluster_radiosity = weighted / cluster_area[None, :]
    source_pack = jnp.concatenate(
        [
            node_position[:, leaf_count:],
            normals[:, leaf_count:],
            cluster_area[None, :],
            cluster_radiosity,
        ],
        axis=0,
    )
    receiver_pack = jnp.concatenate([node_position, normals], axis=0)
    linked = lax.all_to_all(receiver_pack, "dev", split_axis=1, concat_axis=1, tiled=True)
    receiver_tiles = linked.reshape(6, tile_count, TILE)
    everything = lax.all_gather(source_pack, "dev", axis=1, tiled=True)
    source_tiles = everything.reshape(10, -1, TILE)
    receiver_ids = block_receiver[0]
    source_ids = block_source[0]
    live_count = block_count[0, 0]
    step_slots = min(batch_slots, slot_count)

    def add_batch(rounds, totals):
        first = rounds * step_slots
        batch_receivers = lax.dynamic_slice_in_dim(receiver_ids, first, step_slots, 0)
        batch_sources = lax.dynamic_slice_in_dim(source_ids, first, step_slots, 0)
        batch_weight = (first + jnp.arange(step_slots, dtype=jnp.int32) < live_count).astype(
            jnp.float32
        )
        receivers = jnp.take(receiver_tiles, batch_receivers, axis=1)
        sources = jnp.take(source_tiles, batch_sources, axis=1)
        contrib = tile_irradiance(receivers, sources) * batch_weight[:, None, None]
        placement = (
            batch_receivers[:, None] == jnp.arange(tile_count, dtype=jnp.int32)[None, :]
        ).astype(jnp.float32)
        return totals + jnp.einsum(
            "bt,bci->cti", placement, contrib, precision=lax.Precision.HIGHEST
        )

    batch_total = (live_count + step_slots - 1) // step_slots
    totals = lax.fori_loop(0, batch_total, add_batch, jnp.zeros((3, tile_count, TILE), jnp.float32))
    partial_value = totals.reshape(3, node_count)
    summed = lax.psum(partial_value, "grp")
    irradiance = lax.all_to_all(summed, "dev", split_axis=1, concat_axis=1, tiled=True)
    pushed = jnp.dot(irradiance[:, leaf_count:], parent_onehot.T, precision=lax.Precision.HIGHEST)
    gathered = irradiance[:, :leaf_count] + pushed
    return leaf_emit + leaf_albedo * gathered


F32 = jnp.float32
BF16 = jnp.bfloat16
MESH = pl.DeviceIdType.MESH
NT_DIMS = (((1,), (1,)), ((), ()))
FEATURES = 8
RELAY_TURN = 4
ROWS = 64


def split3(values):
    high = values.astype(BF16).astype(F32)
    rest = values - high
    middle = rest.astype(BF16).astype(F32)
    return high, middle, rest - middle


def stack3(values):
    rows = values.shape[0]
    pad = jnp.zeros((16 - 3 * rows, values.shape[1]), F32)
    return jnp.concatenate(list(split3(values)) + [pad], axis=0).astype(BF16)


def unstack3(product, rows):
    return product[0:rows] + product[rows : 2 * rows] + product[2 * rows : 3 * rows]


def flip(k, turn, shards):
    value, bit = 0, 1
    while bit < shards:
        digit = k // bit % 2
        value = value + bit * ((1 - digit) if turn // bit % 2 else digit)
        bit *= 2
    return value


def all_bits(g, pattern, groups, wanted):
    value, bit = 1, 1
    while bit < groups:
        if pattern // bit % 2:
            digit = g // bit % 2
            value = value * (digit if wanted else 1 - digit)
        bit *= 2
    return value


def paired_rows(left, const):
    one, two, three = split3(left)
    row = lax.broadcasted_iota(jnp.int32, left.shape, 0)
    free = (row == 6) | (row == 7)
    plain = [jnp.where(free, 0.0, part) for part in (one, two, three)]
    zero = jnp.zeros_like(left)
    c1, c2, c3 = [zero] * 3 if const is None else split3(jnp.broadcast_to(const, left.shape))
    at6 = row == 6
    with_sum = jnp.where(free, left, one)
    return jnp.concatenate(
        [
            with_sum,
            jnp.where(at6, c1, plain[1]),
            jnp.where(at6, c2, plain[2]),
            with_sum,
            jnp.where(at6, c3, plain[1]),
            with_sum,
        ],
        axis=0,
    ).astype(BF16)


def dense_kernel(groups, shards, *refs):
    operands, count, out, inputs, scratch = refs[:7], refs[7], refs[8], refs[9:16], refs[16:]
    receiver_id, source_id, radiosity, area, parent, position, angles = inputs
    (
        load,
        sources, my_pack, my_hist, hists, right, onehot, place, columns, turned, sums,
        src_send, src_recv, hist_send, hist_recv, pass_send, peer_recv,
    ) = scratch
    g = lax.axis_index("grp")
    k = lax.axis_index("dev")
    device_total = groups * shards
    me = g * shards + k
    leaves = radiosity.shape[1]
    nodes = position.shape[1]
    clusters = nodes - leaves
    per_shard = clusters // TILE
    source_tiles = shards * per_shard
    per_peer = nodes // shards
    chunks = nodes // TILE
    pairs = nodes // (2 * TILE)

    loads = [
        pltpu.make_async_copy(operands[i], inputs[i], load.at[i]) for i in range(len(inputs))
    ]
    for copy in loads:
        copy.start()

    barrier = pltpu.get_barrier_semaphore()
    far_first = sorted(range(shards), key=lambda step: -step)
    group = [flip(g, e, groups) for e in range(groups)]
    drops = [all_bits(g, e, groups, True) for e in range(groups)]
    clear = [all_bits(g, e, groups, False) for e in range(groups)]

    def greet(e, shard):
        pl.semaphore_signal(
            barrier, inc=1, device_id=(group[e], shard), device_id_type=MESH
        )

    for e in reversed(range(groups)):

        @pl.when(clear[e] == 1)
        def _():
            lax.fori_loop(0, k, lambda shard, _: (greet(e, shard), 0)[1], 0)

        lax.fori_loop(k + 1, shards, lambda shard, _: (greet(e, shard), 0)[1], 0)
        if e:
            greet(e, k)

    for copy in loads:
        copy.wait()

    lane = lax.broadcasted_iota(jnp.int32, (1, TILE), 1)
    code = jnp.where(
        lane < count[0, 0], receiver_id[...] * source_tiles + source_id[...], -1
    )
    square = lax.broadcasted_iota(jnp.int32, (TILE, TILE), 0)
    hit = jnp.where(square == code, 1.0, 0.0).astype(BF16)
    counted = lax.dot_general(
        jnp.ones((16, TILE), BF16), hit, NT_DIMS, preferred_element_type=F32
    )
    my_hist[...] = counted[0:1]
    hists[me] = counted[0:1]

    ids = lax.broadcasted_iota(jnp.int32, (clusters, leaves), 0)
    onehot[...] = jnp.where(ids == parent[...], 1.0, 0.0).astype(BF16)
    area_row = area[...]
    stacked = stack3(jnp.concatenate([area_row, radiosity[...] * area_row], axis=0))
    cluster = unstack3(
        lax.dot_general(stacked, onehot[...], NT_DIMS, preferred_element_type=F32), 4
    )
    cosines = jnp.cos(angles[...])
    sines = jnp.sin(angles[...])
    normals = jnp.concatenate(
        [cosines[0:1] * cosines[1:2], sines[0:1] * cosines[1:2], sines[1:2]], axis=0
    )
    first_band = cluster[1:2] * (1.0 / jnp.pi)
    facing = normals[:, leaves:] * first_band
    ratios = cluster[2:4] / cluster[1:2]
    for half in range(per_shard):
        here = slice(half * TILE, (half + 1) * TILE)
        there = slice(leaves + half * TILE, leaves + (half + 1) * TILE)
        my_pack[8 * half : 8 * half + 8, :] = jnp.concatenate(
            [position[:, there], facing[:, here], cluster[0:1, here], ratios[0:1, here]], axis=0
        )
        my_pack[8 * per_shard + half : 8 * per_shard + half + 1, :] = ratios[1:2, here]

    drop_total = sum(drops[1:], 1)
    pl.semaphore_wait(barrier, groups - 1 + groups * k + (shards - 1 - k) * drop_total)

    def hist_copy(e, shard):
        return pltpu.make_async_remote_copy(
            src_ref=my_hist,
            dst_ref=hists.at[me],
            send_sem=hist_send.at[e * shards + shard],
            recv_sem=hist_recv,
            device_id=(group[e], shard),
            device_id_type=MESH,
        )

    def peer_copy(e):
        return pltpu.make_async_remote_copy(
            src_ref=my_hist,
            dst_ref=hists.at[me],
            send_sem=hist_send.at[e * shards + k],
            recv_sem=peer_recv.at[e],
            device_id=(group[e], k),
            device_id_type=MESH,
        )

    def passed_copy(e, shard):
        return pltpu.make_async_remote_copy(
            src_ref=hists.at[group[e] * shards + k],
            dst_ref=hists.at[group[e] * shards + k],
            send_sem=pass_send.at[e * shards + shard],
            recv_sem=hist_recv,
            device_id=(g, shard),
            device_id_type=MESH,
        )

    def source_copy(step):
        return pltpu.make_async_remote_copy(
            src_ref=my_pack,
            dst_ref=sources.at[k],
            send_sem=src_send.at[step - 1],
            recv_sem=src_recv.at[k],
            device_id=(g, flip(k, step, shards)),
            device_id_type=MESH,
        )

    def run(first, last, action):
        lax.fori_loop(first, last, lambda shard, _: (action(shard), 0)[1], 0)

    for e in reversed(range(groups)):
        run(0, k, lambda shard: hist_copy(e, shard).start())
    for step in far_first:
        if step:
            source_copy(step).start()
    for e in range(1, groups):
        peer_copy(e).start()
    for e in range(groups):

        @pl.when(drops[e] == 1)
        def _():
            run(k + 1, shards, lambda shard: hist_copy(e, shard).start())

    middle = jnp.sum(position[...], axis=1, keepdims=True) * (1.0 / nodes)
    centred = position[...] - middle
    ones = jnp.ones((1, nodes), F32)
    none = jnp.zeros((1, nodes), F32)
    three = jnp.zeros((3, nodes), F32)
    offset = -jnp.sum(normals * centred, axis=0, keepdims=True)
    norm = jnp.sum(centred * centred, axis=0, keepdims=True)
    for which, rows in enumerate(
        (
            paired_rows(jnp.concatenate([normals, three, none, none], axis=0), offset),
            paired_rows(jnp.concatenate([three, centred, -ones, none], axis=0), None),
            paired_rows(jnp.concatenate([-2.0 * centred, three, none, ones], axis=0), norm),
        )
    ):
        right[which] = rows

    node = lax.broadcasted_iota(jnp.int32, (1, nodes), 1)
    link = jnp.zeros((1, nodes), jnp.int32)
    for j in range(1, shards):
        link += jnp.where(node >= j * per_peer, 1, 0)
    spot = k * per_peer + node - link * per_peer
    low_tile = k * per_peer // TILE
    high_tile = (k * per_peer + per_peer - 1) // TILE
    upper = spot >= (low_tile + 1) * TILE
    owner_row = lax.broadcasted_iota(jnp.int32, (device_total, nodes), 0) % shards
    hits = owner_row == link
    place[0] = jnp.where(hits & ~upper, 1.0, 0.0).astype(BF16)
    place[1] = jnp.where(hits & upper, 1.0, 0.0).astype(BF16)

    row8 = lax.broadcasted_iota(jnp.int32, (8, TILE), 0)
    centre8 = jnp.concatenate([middle, jnp.zeros((5, 1), F32)], axis=0)

    def tile_sums(pack, half, tile):
        values = pack[8 * half : 8 * half + 8, :]
        ratio = pack[8 * per_shard + half : 8 * per_shard + half + 1, :]
        area_here = values[6:7]
        shifted = values - centre8
        spots, aims = shifted[0:3], shifted[3:6]
        along = jnp.sum(spots * aims, axis=0, keepdims=True)
        reach = jnp.sum(spots * spots, axis=0, keepdims=True) + area_here
        one, two, low = split3(jnp.concatenate([spots, aims, along, reach], axis=0))
        left = jnp.concatenate(
            [
                one,
                jnp.where(row8 == 6, 1.0, one),
                jnp.where(row8 == 6, 1.0, one),
                two,
                jnp.where(row8 == 6, 1.0, two),
                low,
            ],
            axis=0,
        )
        extra = jnp.concatenate(
            [values[7:8], ratio, area_here * ((jnp.pi - 1.0) / jnp.pi), jnp.zeros((5, TILE), F32)],
            axis=0,
        )
        features = jnp.transpose(left).astype(BF16)
        column = jnp.transpose(extra)
        second, third, less = [
            jnp.broadcast_to(column[:, i : i + 1], (TILE, TILE)) for i in range(3)
        ]
        for pair in range(pairs):
            wide = slice(pair * 2 * TILE, (pair + 1) * 2 * TILE)
            totals = [[None] * 3, [None] * 3]
            for first in range(0, TILE, ROWS):
                some = slice(first, first + ROWS)
                toward, facing, span = [
                    jnp.dot(features[some], right[which, :, wide], preferred_element_type=F32)
                    for which in range(3)
                ]
                for side in range(2):
                    lanes = slice(side * TILE, (side + 1) * TILE)
                    u = span[:, lanes]
                    form = (
                        jnp.maximum(toward[:, lanes], 0.0)
                        * jnp.maximum(facing[:, lanes], 0.0)
                        / (u * (u - less[some]))
                    )
                    for c, scaled in enumerate((form, form * second[some], form * third[some])):
                        part = jnp.sum(scaled.reshape(ROWS // 8, 8, TILE), axis=0)
                        old = totals[side][c]
                        totals[side][c] = part if old is None else old + part
            for side in range(2):
                first = pair * 2 * TILE + side * TILE
                for c in range(3):
                    sums[tile, c : c + 1, first : first + TILE] = jnp.sum(
                        totals[side][c], axis=0, keepdims=True
                    )

    for first in range(0, shards, 2):
        if first == RELAY_TURN:
            for e in range(1, groups):
                pltpu.make_async_remote_copy(
                    src_ref=my_hist,
                    dst_ref=hists.at[group[e] * shards + k],
                    send_sem=hist_send.at[0],
                    recv_sem=peer_recv.at[e],
                    device_id=(group[e], k),
                    device_id_type=MESH,
                ).wait_recv()

                @pl.when(clear[e] == 0)
                def _():
                    run(k + 1, shards, lambda shard: passed_copy(e, shard).start())

        if first == shards - 2:
            for e in range(groups):
                run(0, k, lambda shard: hist_copy(e, shard).wait_send())

                @pl.when(drops[e] == 1)
                def _():
                    run(k + 1, shards, lambda shard: hist_copy(e, shard).wait_send())

                if e:
                    peer_copy(e).wait_send()

                    @pl.when(clear[e] == 0)
                    def _():
                        run(k + 1, shards, lambda shard: passed_copy(e, shard).wait_send())

            for step in far_first:
                if step:
                    source_copy(step).wait_send()
        packs = []
        for turn in (first, first + 1):
            owner = flip(k, turn, shards)
            if turn:
                pltpu.make_async_remote_copy(
                    src_ref=my_pack,
                    dst_ref=sources.at[owner],
                    send_sem=src_send.at[0],
                    recv_sem=src_recv.at[owner],
                    device_id=(g, owner),
                    device_id_type=MESH,
                ).wait_recv()
            packs.append((sources.at[owner] if turn else my_pack, owner))
        for pack, owner in packs:
            for half in range(per_shard):
                tile_sums(pack, half, owner * per_shard + half)

    distant = hists.at[pl.ds(0, groups * (shards - 1))]
    pltpu.make_async_copy(distant, distant, hist_recv).wait()
    table = jnp.concatenate([hists[d] for d in range(device_total)], axis=0)
    turned[...] = jnp.transpose(table)
    weight = jnp.zeros((source_tiles, nodes), F32)
    for which, tile in enumerate((low_tile, high_tile)):
        rows = turned[pl.ds(pl.multiple_of(tile * source_tiles, 8), source_tiles), :]
        weight += jnp.dot(rows.astype(BF16), place[which], preferred_element_type=F32)

    irradiance = weight[0:1] * sums[0]
    for tile in range(1, source_tiles):
        irradiance += weight[tile : tile + 1] * sums[tile]
    pushed = unstack3(
        jnp.dot(stack3(irradiance[:, leaves:]), onehot[...], preferred_element_type=F32), 3
    )
    out[...] = irradiance[:, :leaves] + pushed


def dense_body(
    groups, shards, leaf_emit, leaf_albedo, leaf_radiosity, leaf_area, parent_index,
    node_position, node_angles, block_receiver, block_source, block_count,
):
    leaves = leaf_area.shape[0]
    nodes = node_position.shape[1]
    clusters = nodes - leaves
    per_shard = clusters // TILE
    source_tiles = shards * per_shard
    device_total = groups * shards
    operands = (
        block_receiver, block_source, leaf_radiosity, leaf_area[None, :], parent_index[None, :],
        node_position, node_angles,
    )
    pack_rows = 9 * per_shard
    gathered = pl.pallas_call(
        functools.partial(dense_kernel, groups, shards),
        out_shape=pltpu.VMEM((3, leaves), F32),
        in_specs=[pl.BlockSpec(memory_space=pltpu.HBM)] * len(operands)
        + [pl.BlockSpec(memory_space=pltpu.SMEM)],
        out_specs=pl.BlockSpec(memory_space=pltpu.VMEM),
        scratch_shapes=[pltpu.VMEM(x.shape, x.dtype) for x in operands]
        + [
            pltpu.SemaphoreType.DMA((len(operands),)),
            pltpu.VMEM((shards, pack_rows, TILE), F32),
            pltpu.VMEM((pack_rows, TILE), F32),
            pltpu.VMEM((1, TILE), F32),
            pltpu.VMEM((device_total, 1, TILE), F32),
            pltpu.VMEM((3, 6 * FEATURES, nodes), BF16),
            pltpu.VMEM((clusters, leaves), BF16),
            pltpu.VMEM((2, device_total, nodes), BF16),
            pltpu.VMEM((TILE, TILE), F32),
            pltpu.VMEM((TILE, device_total), F32),
            pltpu.VMEM((source_tiles, 3, nodes), F32),
            pltpu.SemaphoreType.DMA((shards - 1,)),
            pltpu.SemaphoreType.DMA((shards,)),
            pltpu.SemaphoreType.DMA((device_total,)),
            pltpu.SemaphoreType.DMA,
            pltpu.SemaphoreType.DMA((device_total,)),
            pltpu.SemaphoreType.DMA((groups,)),
        ],
        compiler_params=pltpu.CompilerParams(collective_id=0, has_side_effects=True),
    )(*operands, block_count)
    return leaf_emit + leaf_albedo * gathered


def body(groups, shards, *args):
    leaves, nodes, slots = args[3].shape[0], args[5].shape[1], args[7].shape[1]
    per_shard = (nodes - leaves) // TILE
    source_tiles = shards * per_shard
    dense = (
        nodes // TILE * source_tiles <= TILE
        and TILE % source_tiles == 0
        and source_tiles % 8 == 0
        and nodes % (2 * TILE) == 0
        and nodes % shards == 0
        and nodes // shards <= TILE
        and shards & (shards - 1) == 0
        and shards % 2 == 0
        and groups & (groups - 1) == 0
        and groups * shards <= TILE
        and slots == TILE
    )
    return dense_body(groups, shards, *args) if dense else listed_body(*args)


def solution(mesh):
    in_specs = (
        P(None, "dev"),
        P(None, "dev"),
        P(None, "dev"),
        P("dev"),
        P("dev"),
        P(None, "dev"),
        P(None, "dev"),
        P("grp", "dev"),
        P("grp", "dev"),
        P("grp", "dev"),
    )
    out_specs = P(None, "dev")
    sized = functools.partial(body, mesh.shape["grp"], mesh.shape["dev"])
    return jax.shard_map(sized, mesh=mesh, in_specs=in_specs, out_specs=out_specs, check_vma=False)
```

```python
import functools
import jax
import jax.numpy as jnp
from jax import lax
from jax.experimental import pallas as pl
from jax.experimental.pallas import tpu as pltpu
from jax.sharding import PartitionSpec as P

TILE = 128


batch_slots = 16


def unit_normals(node_angles):
    azimuth = node_angles[0]
    elevation = node_angles[1]
    return jnp.stack(
        [
            jnp.cos(azimuth) * jnp.cos(elevation),
            jnp.sin(azimuth) * jnp.cos(elevation),
            jnp.sin(elevation),
        ]
    )


def tile_irradiance(receivers, sources):
    offsets = [
        sources[axis_id][:, None, :] - receivers[axis_id][:, :, None] for axis_id in range(3)
    ]
    distance_sq = offsets[0] * offsets[0] + offsets[1] * offsets[1] + offsets[2] * offsets[2]
    facing_receiver = (
        receivers[3][:, :, None] * offsets[0]
        + receivers[4][:, :, None] * offsets[1]
        + receivers[5][:, :, None] * offsets[2]
    )
    facing_source = (
        sources[3][:, None, :] * offsets[0]
        + sources[4][:, None, :] * offsets[1]
        + sources[5][:, None, :] * offsets[2]
    )
    source_area = sources[6][:, None, :]
    factor = (
        source_area
        * jnp.maximum(facing_receiver, 0.0)
        * jnp.maximum(-facing_source, 0.0)
        / ((distance_sq + source_area) * (jnp.pi * distance_sq + source_area))
    )
    return jnp.einsum("bij,cbj->bci", factor, sources[7:10], precision=lax.Precision.HIGHEST)


def listed_body(
    leaf_emit,
    leaf_albedo,
    leaf_radiosity,
    leaf_area,
    parent_index,
    node_position,
    node_angles,
    block_receiver,
    block_source,
    block_count,
):
    leaf_count = leaf_area.shape[0]
    node_count = node_position.shape[1]
    cluster_count = node_count - leaf_count
    tile_count = node_count // TILE
    slot_count = block_receiver.shape[1]
    normals = unit_normals(node_angles)
    parent_onehot = (
        parent_index[:, None] == jnp.arange(cluster_count, dtype=jnp.int32)[None, :]
    ).astype(jnp.float32)
    cluster_area = jnp.dot(leaf_area, parent_onehot, precision=lax.Precision.HIGHEST)
    weighted = jnp.dot(
        leaf_radiosity * leaf_area[None, :], parent_onehot, precision=lax.Precision.HIGHEST
    )
    cluster_radiosity = weighted / cluster_area[None, :]
    source_pack = jnp.concatenate(
        [
            node_position[:, leaf_count:],
            normals[:, leaf_count:],
            cluster_area[None, :],
            cluster_radiosity,
        ],
        axis=0,
    )
    receiver_pack = jnp.concatenate([node_position, normals], axis=0)
    linked = lax.all_to_all(receiver_pack, "dev", split_axis=1, concat_axis=1, tiled=True)
    receiver_tiles = linked.reshape(6, tile_count, TILE)
    everything = lax.all_gather(source_pack, "dev", axis=1, tiled=True)
    source_tiles = everything.reshape(10, -1, TILE)
    receiver_ids = block_receiver[0]
    source_ids = block_source[0]
    live_count = block_count[0, 0]
    step_slots = min(batch_slots, slot_count)

    def add_batch(rounds, totals):
        first = rounds * step_slots
        batch_receivers = lax.dynamic_slice_in_dim(receiver_ids, first, step_slots, 0)
        batch_sources = lax.dynamic_slice_in_dim(source_ids, first, step_slots, 0)
        batch_weight = (first + jnp.arange(step_slots, dtype=jnp.int32) < live_count).astype(
            jnp.float32
        )
        receivers = jnp.take(receiver_tiles, batch_receivers, axis=1)
        sources = jnp.take(source_tiles, batch_sources, axis=1)
        contrib = tile_irradiance(receivers, sources) * batch_weight[:, None, None]
        placement = (
            batch_receivers[:, None] == jnp.arange(tile_count, dtype=jnp.int32)[None, :]
        ).astype(jnp.float32)
        return totals + jnp.einsum(
            "bt,bci->cti", placement, contrib, precision=lax.Precision.HIGHEST
        )

    batch_total = (live_count + step_slots - 1) // step_slots
    totals = lax.fori_loop(0, batch_total, add_batch, jnp.zeros((3, tile_count, TILE), jnp.float32))
    partial_value = totals.reshape(3, node_count)
    summed = lax.psum(partial_value, "grp")
    irradiance = lax.all_to_all(summed, "dev", split_axis=1, concat_axis=1, tiled=True)
    pushed = jnp.dot(irradiance[:, leaf_count:], parent_onehot.T, precision=lax.Precision.HIGHEST)
    gathered = irradiance[:, :leaf_count] + pushed
    return leaf_emit + leaf_albedo * gathered


F32 = jnp.float32
BF16 = jnp.bfloat16
MESH = pl.DeviceIdType.MESH
NT_DIMS = (((1,), (1,)), ((), ()))
FEATURES = 8
RELAY_TURN = 4
ROWS = 64


def split3(values):
    high = values.astype(BF16).astype(F32)
    rest = values - high
    middle = rest.astype(BF16).astype(F32)
    return high, middle, rest - middle


def stack3(values):
    rows = values.shape[0]
    pad = jnp.zeros((16 - 3 * rows, values.shape[1]), F32)
    return jnp.concatenate(list(split3(values)) + [pad], axis=0).astype(BF16)


def unstack3(product, rows):
    return product[0:rows] + product[rows : 2 * rows] + product[2 * rows : 3 * rows]


def flip(k, turn, shards):
    value, bit = 0, 1
    while bit < shards:
        digit = k // bit % 2
        value = value + bit * ((1 - digit) if turn // bit % 2 else digit)
        bit *= 2
    return value


def all_bits(g, pattern, groups, wanted):
    value, bit = 1, 1
    while bit < groups:
        if pattern // bit % 2:
            digit = g // bit % 2
            value = value * (digit if wanted else 1 - digit)
        bit *= 2
    return value


def paired_rows(left, const):
    one, two, three = split3(left)
    row = lax.broadcasted_iota(jnp.int32, left.shape, 0)
    free = (row == 6) | (row == 7)
    plain = [jnp.where(free, 0.0, part) for part in (one, two, three)]
    zero = jnp.zeros_like(left)
    c1, c2, c3 = [zero] * 3 if const is None else split3(jnp.broadcast_to(const, left.shape))
    at6 = row == 6
    with_sum = jnp.where(free, left, one)
    return jnp.concatenate(
        [
            with_sum,
            jnp.where(at6, c1, plain[1]),
            jnp.where(at6, c2, plain[2]),
            with_sum,
            jnp.where(at6, c3, plain[1]),
            with_sum,
        ],
        axis=0,
    ).astype(BF16)


def dense_kernel(groups, shards, *refs):
    operands, count, out, inputs, scratch = refs[:7], refs[7], refs[8], refs[9:16], refs[16:]
    receiver_id, source_id, radiosity, area, parent, position, angles = inputs
    (
        load,
        sources, my_pack, my_hist, hists, right, onehot, place, columns, turned, sums,
        src_send, src_recv, hist_send, hist_recv, pass_send, peer_recv,
    ) = scratch
    g = lax.axis_index("grp")
    k = lax.axis_index("dev")
    device_total = groups * shards
    me = g * shards + k
    leaves = radiosity.shape[1]
    nodes = position.shape[1]
    clusters = nodes - leaves
    per_shard = clusters // TILE
    source_tiles = shards * per_shard
    per_peer = nodes // shards
    chunks = nodes // TILE
    pairs = nodes // (2 * TILE)

    loads = [
        pltpu.make_async_copy(operands[i], inputs[i], load.at[i]) for i in range(len(inputs))
    ]
    for copy in loads:
        copy.start()

    barrier = pltpu.get_barrier_semaphore()
    far_first = sorted(range(shards), key=lambda step: -step)
    group = [flip(g, e, groups) for e in range(groups)]
    drops = [all_bits(g, e, groups, True) for e in range(groups)]
    clear = [all_bits(g, e, groups, False) for e in range(groups)]

    def greet(e, shard):
        pl.semaphore_signal(
            barrier, inc=1, device_id=(group[e], shard), device_id_type=MESH
        )

    def run(first, last, action):
        lax.fori_loop(first, last, lambda shard, _: (action(shard), 0)[1], 0)

    for e in range(groups):
        if e:
            greet(e, k)

            @pl.when(clear[e] == 1)
            def _():
                run(0, k, lambda shard: greet(e, shard))

        else:
            run(0, k, lambda shard: greet(0, shard))
        run(k + 1, shards, lambda shard: greet(e, shard))

    for copy in loads:
        copy.wait()

    lane = lax.broadcasted_iota(jnp.int32, (1, TILE), 1)
    code = jnp.where(
        lane < count[0, 0], receiver_id[...] * source_tiles + source_id[...], -1
    )
    square = lax.broadcasted_iota(jnp.int32, (TILE, TILE), 0)
    hit = jnp.where(square == code, 1.0, 0.0).astype(BF16)
    counted = lax.dot_general(
        jnp.ones((16, TILE), BF16), hit, NT_DIMS, preferred_element_type=F32
    )
    my_hist[...] = counted[0:1]
    hists[me] = counted[0:1]

    ids = lax.broadcasted_iota(jnp.int32, (clusters, leaves), 0)
    onehot[...] = jnp.where(ids == parent[...], 1.0, 0.0).astype(BF16)
    area_row = area[...]
    stacked = stack3(jnp.concatenate([area_row, radiosity[...] * area_row], axis=0))
    cluster = unstack3(
        lax.dot_general(stacked, onehot[...], NT_DIMS, preferred_element_type=F32), 4
    )
    cosines = jnp.cos(angles[...])
    sines = jnp.sin(angles[...])
    normals = jnp.concatenate(
        [cosines[0:1] * cosines[1:2], sines[0:1] * cosines[1:2], sines[1:2]], axis=0
    )
    first_band = cluster[1:2] * (1.0 / jnp.pi)
    facing = normals[:, leaves:] * first_band
    ratios = cluster[2:4] / cluster[1:2]
    for half in range(per_shard):
        here = slice(half * TILE, (half + 1) * TILE)
        there = slice(leaves + half * TILE, leaves + (half + 1) * TILE)
        my_pack[8 * half : 8 * half + 8, :] = jnp.concatenate(
            [position[:, there], facing[:, here], cluster[0:1, here], ratios[0:1, here]], axis=0
        )
        my_pack[8 * per_shard + half : 8 * per_shard + half + 1, :] = ratios[1:2, here]

    drop_total = sum(drops[1:], 1)
    pl.semaphore_wait(barrier, groups - 1 + groups * k + (shards - 1 - k) * drop_total)

    def hist_copy(e, shard):
        return pltpu.make_async_remote_copy(
            src_ref=my_hist,
            dst_ref=hists.at[me],
            send_sem=hist_send,
            recv_sem=hist_recv,
            device_id=(group[e], shard),
            device_id_type=MESH,
        )

    def peer_copy(e):
        return pltpu.make_async_remote_copy(
            src_ref=my_hist,
            dst_ref=hists.at[me],
            send_sem=hist_send,
            recv_sem=peer_recv.at[e],
            device_id=(group[e], k),
            device_id_type=MESH,
        )

    def passed_copy(e, shard):
        return pltpu.make_async_remote_copy(
            src_ref=hists.at[group[e] * shards + k],
            dst_ref=hists.at[group[e] * shards + k],
            send_sem=pass_send,
            recv_sem=hist_recv,
            device_id=(g, shard),
            device_id_type=MESH,
        )

    def source_copy(step):
        return pltpu.make_async_remote_copy(
            src_ref=my_pack,
            dst_ref=sources.at[k],
            send_sem=src_send,
            recv_sem=src_recv.at[k],
            device_id=(g, flip(k, step, shards)),
            device_id_type=MESH,
        )

    run(0, k, lambda shard: hist_copy(groups - 1, shard).start())
    for step in far_first:
        if step:
            source_copy(step).start()
    for e in reversed(range(groups - 1)):
        run(0, k, lambda shard: hist_copy(e, shard).start())
    for e in range(1, groups):
        peer_copy(e).start()
    for e in range(groups):

        @pl.when(drops[e] == 1)
        def _():
            run(k + 1, shards, lambda shard: hist_copy(e, shard).start())

    middle = jnp.sum(position[...], axis=1, keepdims=True) * (1.0 / nodes)
    centred = position[...] - middle
    ones = jnp.ones((1, nodes), F32)
    none = jnp.zeros((1, nodes), F32)
    three = jnp.zeros((3, nodes), F32)
    offset = -jnp.sum(normals * centred, axis=0, keepdims=True)
    norm = jnp.sum(centred * centred, axis=0, keepdims=True)
    for which, rows in enumerate(
        (
            paired_rows(jnp.concatenate([normals, three, none, none], axis=0), offset),
            paired_rows(jnp.concatenate([three, centred, -ones, none], axis=0), None),
            paired_rows(jnp.concatenate([-2.0 * centred, three, none, ones], axis=0), norm),
        )
    ):
        right[which] = rows

    node = lax.broadcasted_iota(jnp.int32, (1, nodes), 1)
    link = jnp.zeros((1, nodes), jnp.int32)
    for j in range(1, shards):
        link += jnp.where(node >= j * per_peer, 1, 0)
    spot = k * per_peer + node - link * per_peer
    low_tile = k * per_peer // TILE
    high_tile = (k * per_peer + per_peer - 1) // TILE
    upper = spot >= (low_tile + 1) * TILE
    owner_row = lax.broadcasted_iota(jnp.int32, (device_total, nodes), 0) % shards
    hits = owner_row == link
    place[0] = jnp.where(hits & ~upper, 1.0, 0.0).astype(BF16)
    place[1] = jnp.where(hits & upper, 1.0, 0.0).astype(BF16)

    row8 = lax.broadcasted_iota(jnp.int32, (8, TILE), 0)
    centre8 = jnp.concatenate([middle, jnp.zeros((5, 1), F32)], axis=0)

    def prepare(pack, half, tile):
        values = pack[8 * half : 8 * half + 8, :]
        ratio = pack[8 * per_shard + half : 8 * per_shard + half + 1, :]
        area_here = values[6:7]
        shifted = values - centre8
        spots, aims = shifted[0:3], shifted[3:6]
        along = jnp.sum(spots * aims, axis=0, keepdims=True)
        reach = jnp.sum(spots * spots, axis=0, keepdims=True) + area_here
        one, two, low = split3(jnp.concatenate([spots, aims, along, reach], axis=0))
        left = jnp.concatenate(
            [
                one,
                jnp.where(row8 == 6, 1.0, one),
                jnp.where(row8 == 6, 1.0, one),
                two,
                jnp.where(row8 == 6, 1.0, two),
                low,
            ],
            axis=0,
        )
        extra = jnp.concatenate(
            [values[7:8], ratio, area_here * ((jnp.pi - 1.0) / jnp.pi), jnp.zeros((5, TILE), F32)],
            axis=0,
        )
        features = jnp.transpose(left).astype(BF16)
        column = jnp.transpose(extra)
        second, third, less = [
            jnp.broadcast_to(column[:, i : i + 1], (TILE, TILE)) for i in range(3)
        ]
        return features, second, third, less, tile

    def evaluate(features, second, third, less, tile):
        for pair in range(pairs):
            wide = slice(pair * 2 * TILE, (pair + 1) * 2 * TILE)
            totals = [[None] * 3, [None] * 3]
            for first in range(0, TILE, ROWS):
                some = slice(first, first + ROWS)
                toward, facing, span = [
                    jnp.dot(features[some], right[which, :, wide], preferred_element_type=F32)
                    for which in range(3)
                ]
                for side in range(2):
                    lanes = slice(side * TILE, (side + 1) * TILE)
                    u = span[:, lanes]
                    form = (
                        jnp.maximum(toward[:, lanes], 0.0)
                        * jnp.maximum(facing[:, lanes], 0.0)
                        / (u * (u - less[some]))
                    )
                    for c, scaled in enumerate((form, form * second[some], form * third[some])):
                        part = jnp.sum(scaled.reshape(ROWS // 8, 8, TILE), axis=0)
                        old = totals[side][c]
                        totals[side][c] = part if old is None else old + part
            for side in range(2):
                first = pair * 2 * TILE + side * TILE
                for c in range(3):
                    sums[tile, c : c + 1, first : first + TILE] = jnp.sum(
                        totals[side][c], axis=0, keepdims=True
                    )

    def rows_done(rows, semaphore):
        some = hists.at[pl.ds(0, rows)]
        pltpu.make_async_copy(some, some, semaphore).wait()

    def settle():
        everything = sources.at[pl.ds(0, shards - 1)]
        pltpu.make_async_copy(everything, everything, src_send).wait()
        levels = [1]
        while levels[-1] < groups:
            levels.append(2 * levels[-1])
        for shard in range(shards):

            @pl.when(k == shard)
            def _():
                for level in levels:
                    later = shards - 1 - shard
                    rows = groups - 1 + groups * shard + later * level
                    passed = later * (groups - groups // level)

                    @pl.when(drop_total == level)
                    def _():
                        rows_done(rows, hist_send)
                        if passed:
                            rows_done(passed, pass_send)

    def peer_arrival(e):
        pltpu.make_async_remote_copy(
            src_ref=my_hist,
            dst_ref=hists.at[group[e] * shards + k],
            send_sem=hist_send,
            recv_sem=peer_recv.at[e],
            device_id=(group[e], k),
            device_id_type=MESH,
        ).wait_recv()

    held = []
    for first in range(0, shards, 2):
        if first == RELAY_TURN:
            for e in range(1, groups):

                @pl.when(clear[e] == 0)
                def _():
                    peer_arrival(e)
                    run(k + 1, shards, lambda shard: passed_copy(e, shard).start())

        if first == shards - 2:
            settle()
        packs = []
        for turn in (first, first + 1):
            owner = flip(k, turn, shards)
            if turn:
                pltpu.make_async_remote_copy(
                    src_ref=my_pack,
                    dst_ref=sources.at[owner],
                    send_sem=src_send,
                    recv_sem=src_recv.at[owner],
                    device_id=(g, owner),
                    device_id_type=MESH,
                ).wait_recv()
            packs.append((sources.at[owner] if turn else my_pack, owner))
        ready = [
            prepare(pack, half, owner * per_shard + half)
            for pack, owner in packs
            for half in range(per_shard)
        ]
        for tile in held + ready[:-1]:
            evaluate(*tile)
        held = ready[-1:]
    for tile in held:
        evaluate(*tile)

    for e in range(1, groups):

        @pl.when(clear[e] == 1)
        def _():
            peer_arrival(e)

    distant = hists.at[pl.ds(0, groups * (shards - 1))]
    pltpu.make_async_copy(distant, distant, hist_recv).wait()
    table = jnp.concatenate([hists[d] for d in range(device_total)], axis=0)
    turned[...] = jnp.transpose(table)
    weight = jnp.zeros((source_tiles, nodes), F32)
    for which, tile in enumerate((low_tile, high_tile)):
        rows = turned[pl.ds(pl.multiple_of(tile * source_tiles, 8), source_tiles), :]
        weight += jnp.dot(rows.astype(BF16), place[which], preferred_element_type=F32)

    irradiance = weight[0:1] * sums[0]
    for tile in range(1, source_tiles):
        irradiance += weight[tile : tile + 1] * sums[tile]
    pushed = unstack3(
        jnp.dot(stack3(irradiance[:, leaves:]), onehot[...], preferred_element_type=F32), 3
    )
    out[...] = irradiance[:, :leaves] + pushed


def dense_body(
    groups, shards, leaf_emit, leaf_albedo, leaf_radiosity, leaf_area, parent_index,
    node_position, node_angles, block_receiver, block_source, block_count,
):
    leaves = leaf_area.shape[0]
    nodes = node_position.shape[1]
    clusters = nodes - leaves
    per_shard = clusters // TILE
    source_tiles = shards * per_shard
    device_total = groups * shards
    operands = (
        block_receiver, block_source, leaf_radiosity, leaf_area[None, :], parent_index[None, :],
        node_position, node_angles,
    )
    pack_rows = 9 * per_shard
    gathered = pl.pallas_call(
        functools.partial(dense_kernel, groups, shards),
        out_shape=pltpu.VMEM((3, leaves), F32),
        in_specs=[pl.BlockSpec(memory_space=pltpu.HBM)] * len(operands)
        + [pl.BlockSpec(memory_space=pltpu.SMEM)],
        out_specs=pl.BlockSpec(memory_space=pltpu.VMEM),
        scratch_shapes=[pltpu.VMEM(x.shape, x.dtype) for x in operands]
        + [
            pltpu.SemaphoreType.DMA((len(operands),)),
            pltpu.VMEM((shards, pack_rows, TILE), F32),
            pltpu.VMEM((pack_rows, TILE), F32),
            pltpu.VMEM((1, TILE), F32),
            pltpu.VMEM((device_total, 1, TILE), F32),
            pltpu.VMEM((3, 6 * FEATURES, nodes), BF16),
            pltpu.VMEM((clusters, leaves), BF16),
            pltpu.VMEM((2, device_total, nodes), BF16),
            pltpu.VMEM((TILE, TILE), F32),
            pltpu.VMEM((TILE, device_total), F32),
            pltpu.VMEM((source_tiles, 3, nodes), F32),
            pltpu.SemaphoreType.DMA,
            pltpu.SemaphoreType.DMA((shards,)),
            pltpu.SemaphoreType.DMA,
            pltpu.SemaphoreType.DMA,
            pltpu.SemaphoreType.DMA,
            pltpu.SemaphoreType.DMA((groups,)),
        ],
        compiler_params=pltpu.CompilerParams(collective_id=0, has_side_effects=True),
    )(*operands, block_count)
    return leaf_emit + leaf_albedo * gathered


def body(groups, shards, *args):
    leaves, nodes, slots = args[3].shape[0], args[5].shape[1], args[7].shape[1]
    per_shard = (nodes - leaves) // TILE
    source_tiles = shards * per_shard
    dense = (
        nodes // TILE * source_tiles <= TILE
        and TILE % source_tiles == 0
        and source_tiles % 8 == 0
        and nodes % (2 * TILE) == 0
        and nodes % shards == 0
        and nodes // shards <= TILE
        and shards & (shards - 1) == 0
        and shards % 2 == 0
        and groups & (groups - 1) == 0
        and groups * shards <= TILE
        and slots == TILE
    )
    return dense_body(groups, shards, *args) if dense else listed_body(*args)


def solution(mesh):
    in_specs = (
        P(None, "dev"),
        P(None, "dev"),
        P(None, "dev"),
        P("dev"),
        P("dev"),
        P(None, "dev"),
        P(None, "dev"),
        P("grp", "dev"),
        P("grp", "dev"),
        P("grp", "dev"),
    )
    out_specs = P(None, "dev")
    sized = functools.partial(body, mesh.shape["grp"], mesh.shape["dev"])
    return jax.shard_map(sized, mesh=mesh, in_specs=in_specs, out_specs=out_specs, check_vma=False)
```

```python
import functools
import jax
import jax.numpy as jnp
from jax import lax
from jax.experimental import pallas as pl
from jax.experimental.pallas import tpu as pltpu
from jax.sharding import PartitionSpec as P

TILE = 128


batch_slots = 16


def unit_normals(node_angles):
    azimuth = node_angles[0]
    elevation = node_angles[1]
    return jnp.stack(
        [
            jnp.cos(azimuth) * jnp.cos(elevation),
            jnp.sin(azimuth) * jnp.cos(elevation),
            jnp.sin(elevation),
        ]
    )


def tile_irradiance(receivers, sources):
    offsets = [
        sources[axis_id][:, None, :] - receivers[axis_id][:, :, None] for axis_id in range(3)
    ]
    distance_sq = offsets[0] * offsets[0] + offsets[1] * offsets[1] + offsets[2] * offsets[2]
    facing_receiver = (
        receivers[3][:, :, None] * offsets[0]
        + receivers[4][:, :, None] * offsets[1]
        + receivers[5][:, :, None] * offsets[2]
    )
    facing_source = (
        sources[3][:, None, :] * offsets[0]
        + sources[4][:, None, :] * offsets[1]
        + sources[5][:, None, :] * offsets[2]
    )
    source_area = sources[6][:, None, :]
    factor = (
        source_area
        * jnp.maximum(facing_receiver, 0.0)
        * jnp.maximum(-facing_source, 0.0)
        / ((distance_sq + source_area) * (jnp.pi * distance_sq + source_area))
    )
    return jnp.einsum("bij,cbj->bci", factor, sources[7:10], precision=lax.Precision.HIGHEST)


def listed_body(
    leaf_emit,
    leaf_albedo,
    leaf_radiosity,
    leaf_area,
    parent_index,
    node_position,
    node_angles,
    block_receiver,
    block_source,
    block_count,
):
    leaf_count = leaf_area.shape[0]
    node_count = node_position.shape[1]
    cluster_count = node_count - leaf_count
    tile_count = node_count // TILE
    slot_count = block_receiver.shape[1]
    normals = unit_normals(node_angles)
    parent_onehot = (
        parent_index[:, None] == jnp.arange(cluster_count, dtype=jnp.int32)[None, :]
    ).astype(jnp.float32)
    cluster_area = jnp.dot(leaf_area, parent_onehot, precision=lax.Precision.HIGHEST)
    weighted = jnp.dot(
        leaf_radiosity * leaf_area[None, :], parent_onehot, precision=lax.Precision.HIGHEST
    )
    cluster_radiosity = weighted / cluster_area[None, :]
    source_pack = jnp.concatenate(
        [
            node_position[:, leaf_count:],
            normals[:, leaf_count:],
            cluster_area[None, :],
            cluster_radiosity,
        ],
        axis=0,
    )
    receiver_pack = jnp.concatenate([node_position, normals], axis=0)
    linked = lax.all_to_all(receiver_pack, "dev", split_axis=1, concat_axis=1, tiled=True)
    receiver_tiles = linked.reshape(6, tile_count, TILE)
    everything = lax.all_gather(source_pack, "dev", axis=1, tiled=True)
    source_tiles = everything.reshape(10, -1, TILE)
    receiver_ids = block_receiver[0]
    source_ids = block_source[0]
    live_count = block_count[0, 0]
    step_slots = min(batch_slots, slot_count)

    def add_batch(rounds, totals):
        first = rounds * step_slots
        batch_receivers = lax.dynamic_slice_in_dim(receiver_ids, first, step_slots, 0)
        batch_sources = lax.dynamic_slice_in_dim(source_ids, first, step_slots, 0)
        batch_weight = (first + jnp.arange(step_slots, dtype=jnp.int32) < live_count).astype(
            jnp.float32
        )
        receivers = jnp.take(receiver_tiles, batch_receivers, axis=1)
        sources = jnp.take(source_tiles, batch_sources, axis=1)
        contrib = tile_irradiance(receivers, sources) * batch_weight[:, None, None]
        placement = (
            batch_receivers[:, None] == jnp.arange(tile_count, dtype=jnp.int32)[None, :]
        ).astype(jnp.float32)
        return totals + jnp.einsum(
            "bt,bci->cti", placement, contrib, precision=lax.Precision.HIGHEST
        )

    batch_total = (live_count + step_slots - 1) // step_slots
    totals = lax.fori_loop(0, batch_total, add_batch, jnp.zeros((3, tile_count, TILE), jnp.float32))
    partial_value = totals.reshape(3, node_count)
    summed = lax.psum(partial_value, "grp")
    irradiance = lax.all_to_all(summed, "dev", split_axis=1, concat_axis=1, tiled=True)
    pushed = jnp.dot(irradiance[:, leaf_count:], parent_onehot.T, precision=lax.Precision.HIGHEST)
    gathered = irradiance[:, :leaf_count] + pushed
    return leaf_emit + leaf_albedo * gathered


F32 = jnp.float32
BF16 = jnp.bfloat16
MESH = pl.DeviceIdType.MESH
NT_DIMS = (((1,), (1,)), ((), ()))
FEATURES = 8
RELAY_TURN = 4
HELD_PAIRS = 1
ROWS = 64


def split3(values):
    high = values.astype(BF16).astype(F32)
    rest = values - high
    middle = rest.astype(BF16).astype(F32)
    return high, middle, rest - middle


def stack3(values):
    rows = values.shape[0]
    pad = jnp.zeros((16 - 3 * rows, values.shape[1]), F32)
    return jnp.concatenate(list(split3(values)) + [pad], axis=0).astype(BF16)


def unstack3(product, rows):
    return product[0:rows] + product[rows : 2 * rows] + product[2 * rows : 3 * rows]


def flip(k, turn, shards):
    value, bit = 0, 1
    while bit < shards:
        digit = k // bit % 2
        value = value + bit * ((1 - digit) if turn // bit % 2 else digit)
        bit *= 2
    return value


def all_bits(g, pattern, groups, wanted):
    value, bit = 1, 1
    while bit < groups:
        if pattern // bit % 2:
            digit = g // bit % 2
            value = value * (digit if wanted else 1 - digit)
        bit *= 2
    return value


def paired_rows(left, const):
    one, two, three = split3(left)
    row = lax.broadcasted_iota(jnp.int32, left.shape, 0)
    free = (row == 6) | (row == 7)
    plain = [jnp.where(free, 0.0, part) for part in (one, two, three)]
    zero = jnp.zeros_like(left)
    c1, c2, c3 = [zero] * 3 if const is None else split3(jnp.broadcast_to(const, left.shape))
    at6 = row == 6
    with_sum = jnp.where(free, left, one)
    return jnp.concatenate(
        [
            with_sum,
            jnp.where(at6, c1, plain[1]),
            jnp.where(at6, c2, plain[2]),
            with_sum,
            jnp.where(at6, c3, plain[1]),
            with_sum,
        ],
        axis=0,
    ).astype(BF16)


def dense_kernel(groups, shards, *refs):
    operands, count, out, inputs, scratch = refs[:7], refs[7], refs[8], refs[9:16], refs[16:]
    receiver_id, source_id, radiosity, area, parent, position, angles = inputs
    (
        load,
        sources, my_pack, my_hist, hists, right, onehot, place, columns, turned, sums,
        src_send, src_recv, hist_send, hist_recv, pass_send, peer_recv,
    ) = scratch
    g = lax.axis_index("grp")
    k = lax.axis_index("dev")
    device_total = groups * shards
    me = g * shards + k
    leaves = radiosity.shape[1]
    nodes = position.shape[1]
    clusters = nodes - leaves
    per_shard = clusters // TILE
    source_tiles = shards * per_shard
    per_peer = nodes // shards
    chunks = nodes // TILE
    pairs = nodes // (2 * TILE)

    loads = [
        pltpu.make_async_copy(operands[i], inputs[i], load.at[i]) for i in range(len(inputs))
    ]
    for copy in loads:
        copy.start()

    barrier = pltpu.get_barrier_semaphore()
    group = [flip(g, e, groups) for e in range(groups)]
    drops = [all_bits(g, e, groups, True) for e in range(groups)]
    clear = [all_bits(g, e, groups, False) for e in range(groups)]

    def greet(e, shard):
        pl.semaphore_signal(
            barrier, inc=1, device_id=(group[e], shard), device_id_type=MESH
        )

    def run(first, last, action):
        lax.fori_loop(first, last, lambda shard, _: (action(shard), 0)[1], 0)

    for e in range(groups):
        if e:
            greet(e, k)

            @pl.when(clear[e] == 1)
            def _():
                run(0, k, lambda shard: greet(e, shard))

        else:
            run(0, k, lambda shard: greet(0, shard))
        run(k + 1, shards, lambda shard: greet(e, shard))

    for copy in loads:
        copy.wait()

    lane = lax.broadcasted_iota(jnp.int32, (1, TILE), 1)
    code = jnp.where(
        lane < count[0, 0], receiver_id[...] * source_tiles + source_id[...], -1
    )
    square = lax.broadcasted_iota(jnp.int32, (TILE, TILE), 0)
    hit = jnp.where(square == code, 1.0, 0.0).astype(BF16)
    counted = lax.dot_general(
        jnp.ones((16, TILE), BF16), hit, NT_DIMS, preferred_element_type=F32
    )
    my_hist[...] = counted[0:1]
    hists[me] = counted[0:1]

    ids = lax.broadcasted_iota(jnp.int32, (clusters, leaves), 0)
    onehot[...] = jnp.where(ids == parent[...], 1.0, 0.0).astype(BF16)
    area_row = area[...]
    stacked = stack3(jnp.concatenate([area_row, radiosity[...] * area_row], axis=0))
    cluster = unstack3(
        lax.dot_general(stacked, onehot[...], NT_DIMS, preferred_element_type=F32), 4
    )
    cosines = jnp.cos(angles[...])
    sines = jnp.sin(angles[...])
    normals = jnp.concatenate(
        [cosines[0:1] * cosines[1:2], sines[0:1] * cosines[1:2], sines[1:2]], axis=0
    )
    first_band = cluster[1:2] * (1.0 / jnp.pi)
    facing = normals[:, leaves:] * first_band
    ratios = cluster[2:4] / cluster[1:2]
    for half in range(per_shard):
        here = slice(half * TILE, (half + 1) * TILE)
        there = slice(leaves + half * TILE, leaves + (half + 1) * TILE)
        my_pack[8 * half : 8 * half + 8, :] = jnp.concatenate(
            [position[:, there], facing[:, here], cluster[0:1, here], ratios[0:1, here]], axis=0
        )
        my_pack[8 * per_shard + half : 8 * per_shard + half + 1, :] = ratios[1:2, here]

    drop_total = sum(drops[1:], 1)
    pl.semaphore_wait(barrier, groups - 1 + groups * k + (shards - 1 - k) * drop_total)

    def hist_copy(e, shard):
        return pltpu.make_async_remote_copy(
            src_ref=my_hist,
            dst_ref=hists.at[me],
            send_sem=hist_send,
            recv_sem=hist_recv,
            device_id=(group[e], shard),
            device_id_type=MESH,
        )

    def peer_copy(e):
        return pltpu.make_async_remote_copy(
            src_ref=my_hist,
            dst_ref=hists.at[me],
            send_sem=hist_send,
            recv_sem=peer_recv.at[e],
            device_id=(group[e], k),
            device_id_type=MESH,
        )

    def passed_copy(e, shard):
        return pltpu.make_async_remote_copy(
            src_ref=hists.at[group[e] * shards + k],
            dst_ref=hists.at[group[e] * shards + k],
            send_sem=pass_send,
            recv_sem=hist_recv,
            device_id=(g, shard),
            device_id_type=MESH,
        )

    def source_copy(shard):
        return pltpu.make_async_remote_copy(
            src_ref=my_pack,
            dst_ref=sources.at[k],
            send_sem=src_send,
            recv_sem=src_recv.at[k],
            device_id=(g, shard),
            device_id_type=MESH,
        )

    run(0, k, lambda shard: hist_copy(groups - 1, shard).start())
    run(0, k, lambda shard: source_copy(shard).start())
    run(k + 1, shards, lambda shard: source_copy(shard).start())
    for e in reversed(range(groups - 1)):
        run(0, k, lambda shard: hist_copy(e, shard).start())
    for e in range(1, groups):
        peer_copy(e).start()
    for e in range(groups):

        @pl.when(drops[e] == 1)
        def _():
            run(k + 1, shards, lambda shard: hist_copy(e, shard).start())

    middle = jnp.sum(position[...], axis=1, keepdims=True) * (1.0 / nodes)
    centred = position[...] - middle
    ones = jnp.ones((1, nodes), F32)
    none = jnp.zeros((1, nodes), F32)
    three = jnp.zeros((3, nodes), F32)
    offset = -jnp.sum(normals * centred, axis=0, keepdims=True)
    norm = jnp.sum(centred * centred, axis=0, keepdims=True)
    for which, rows in enumerate(
        (
            paired_rows(jnp.concatenate([normals, three, none, none], axis=0), offset),
            paired_rows(jnp.concatenate([three, centred, -ones, none], axis=0), None),
            paired_rows(jnp.concatenate([-2.0 * centred, three, none, ones], axis=0), norm),
        )
    ):
        right[which] = rows

    node = lax.broadcasted_iota(jnp.int32, (1, nodes), 1)
    link = jnp.zeros((1, nodes), jnp.int32)
    for j in range(1, shards):
        link += jnp.where(node >= j * per_peer, 1, 0)
    spot = k * per_peer + node - link * per_peer
    low_tile = k * per_peer // TILE
    high_tile = (k * per_peer + per_peer - 1) // TILE
    upper = spot >= (low_tile + 1) * TILE
    owner_row = lax.broadcasted_iota(jnp.int32, (device_total, nodes), 0) % shards
    hits = owner_row == link
    place[0] = jnp.where(hits & ~upper, 1.0, 0.0).astype(BF16)
    place[1] = jnp.where(hits & upper, 1.0, 0.0).astype(BF16)

    row8 = lax.broadcasted_iota(jnp.int32, (8, TILE), 0)
    centre8 = jnp.concatenate([middle, jnp.zeros((5, 1), F32)], axis=0)

    def prepare(pack, half, tile):
        values = pack[8 * half : 8 * half + 8, :]
        ratio = pack[8 * per_shard + half : 8 * per_shard + half + 1, :]
        area_here = values[6:7]
        shifted = values - centre8
        spots, aims = shifted[0:3], shifted[3:6]
        along = jnp.sum(spots * aims, axis=0, keepdims=True)
        reach = jnp.sum(spots * spots, axis=0, keepdims=True) + area_here
        one, two, low = split3(jnp.concatenate([spots, aims, along, reach], axis=0))
        left = jnp.concatenate(
            [
                one,
                jnp.where(row8 == 6, 1.0, one),
                jnp.where(row8 == 6, 1.0, one),
                two,
                jnp.where(row8 == 6, 1.0, two),
                low,
            ],
            axis=0,
        )
        extra = jnp.concatenate(
            [values[7:8], ratio, area_here * ((jnp.pi - 1.0) / jnp.pi), jnp.zeros((5, TILE), F32)],
            axis=0,
        )
        features = jnp.transpose(left).astype(BF16)
        column = jnp.transpose(extra)
        second, third, less = [
            jnp.broadcast_to(column[:, i : i + 1], (TILE, TILE)) for i in range(3)
        ]
        return features, second, third, less, tile

    def products(features, pair):
        wide = slice(pair * 2 * TILE, (pair + 1) * 2 * TILE)
        return [
            [
                jnp.dot(
                    features[first : first + ROWS], right[which, :, wide],
                    preferred_element_type=F32,
                )
                for which in range(3)
            ]
            for first in range(0, TILE, ROWS)
        ]

    def finish(parts, pair, second, third, less, tile):
        totals = [[None] * 3, [None] * 3]
        for first, (toward, facing, span) in zip(range(0, TILE, ROWS), parts):
            some = slice(first, first + ROWS)
            for side in range(2):
                lanes = slice(side * TILE, (side + 1) * TILE)
                u = span[:, lanes]
                form = (
                    jnp.maximum(toward[:, lanes], 0.0)
                    * jnp.maximum(facing[:, lanes], 0.0)
                    / (u * (u - less[some]))
                )
                for c, scaled in enumerate((form, form * second[some], form * third[some])):
                    part = jnp.sum(scaled.reshape(ROWS // 8, 8, TILE), axis=0)
                    old = totals[side][c]
                    totals[side][c] = part if old is None else old + part
        for side in range(2):
            first = pair * 2 * TILE + side * TILE
            for c in range(3):
                sums[tile, c : c + 1, first : first + TILE] = jnp.sum(
                    totals[side][c], axis=0, keepdims=True
                )

    def rows_done(rows, semaphore):
        some = hists.at[pl.ds(0, rows)]
        pltpu.make_async_copy(some, some, semaphore).wait()

    def settle():
        everything = sources.at[pl.ds(0, shards - 1)]
        pltpu.make_async_copy(everything, everything, src_send).wait()
        levels = [1]
        while levels[-1] < groups:
            levels.append(2 * levels[-1])
        for shard in range(shards):

            @pl.when(k == shard)
            def _():
                for level in levels:
                    later = shards - 1 - shard
                    rows = groups - 1 + groups * shard + later * level
                    passed = later * (groups - groups // level)

                    @pl.when(drop_total == level)
                    def _():
                        rows_done(rows, hist_send)
                        if passed:
                            rows_done(passed, pass_send)

    def peer_arrival(e):
        pltpu.make_async_remote_copy(
            src_ref=my_hist,
            dst_ref=hists.at[group[e] * shards + k],
            send_sem=hist_send,
            recv_sem=peer_recv.at[e],
            device_id=(group[e], k),
            device_id_type=MESH,
        ).wait_recv()

    held = []
    for first in range(0, shards, 2):
        if first == RELAY_TURN:
            for e in range(1, groups):

                @pl.when(clear[e] == 0)
                def _():
                    peer_arrival(e)
                    run(k + 1, shards, lambda shard: passed_copy(e, shard).start())

        if first == shards - 2:
            settle()
        packs = []
        for turn in (first, first + 1):
            owner = flip(k, turn, shards)
            if turn:
                pltpu.make_async_remote_copy(
                    src_ref=my_pack,
                    dst_ref=sources.at[owner],
                    send_sem=src_send,
                    recv_sem=src_recv.at[owner],
                    device_id=(g, owner),
                    device_id_type=MESH,
                ).wait_recv()
            packs.append((sources.at[owner] if turn else my_pack, owner))
        ready = [
            prepare(pack, half, owner * per_shard + half)
            for pack, owner in packs
            for half in range(per_shard)
        ]
        for work in held:
            finish(*work)
        held = []
        for number, (features, *rest) in enumerate(ready):
            for pair in range(pairs):
                work = (products(features, pair), pair, *rest)
                if number == len(ready) - 1 and pair >= pairs - HELD_PAIRS:
                    held.append(work)
                else:
                    finish(*work)

    for e in range(1, groups):

        @pl.when(clear[e] == 1)
        def _():
            peer_arrival(e)

    distant = hists.at[pl.ds(0, groups * (shards - 1))]
    pltpu.make_async_copy(distant, distant, hist_recv).wait()
    table = jnp.concatenate([hists[d] for d in range(device_total)], axis=0)
    turned[...] = jnp.transpose(table)
    weight = jnp.zeros((source_tiles, nodes), F32)
    for which, tile in enumerate((low_tile, high_tile)):
        rows = turned[pl.ds(pl.multiple_of(tile * source_tiles, 8), source_tiles), :]
        weight += jnp.dot(rows.astype(BF16), place[which], preferred_element_type=F32)
    for work in held:
        finish(*work)

    irradiance = weight[0:1] * sums[0]
    for tile in range(1, source_tiles):
        irradiance += weight[tile : tile + 1] * sums[tile]
    pushed = unstack3(
        jnp.dot(stack3(irradiance[:, leaves:]), onehot[...], preferred_element_type=F32), 3
    )
    out[...] = irradiance[:, :leaves] + pushed


def dense_body(
    groups, shards, leaf_emit, leaf_albedo, leaf_radiosity, leaf_area, parent_index,
    node_position, node_angles, block_receiver, block_source, block_count,
):
    leaves = leaf_area.shape[0]
    nodes = node_position.shape[1]
    clusters = nodes - leaves
    per_shard = clusters // TILE
    source_tiles = shards * per_shard
    device_total = groups * shards
    operands = (
        block_receiver, block_source, leaf_radiosity, leaf_area[None, :], parent_index[None, :],
        node_position, node_angles,
    )
    pack_rows = 9 * per_shard
    gathered = pl.pallas_call(
        functools.partial(dense_kernel, groups, shards),
        out_shape=pltpu.VMEM((3, leaves), F32),
        in_specs=[pl.BlockSpec(memory_space=pltpu.HBM)] * len(operands)
        + [pl.BlockSpec(memory_space=pltpu.SMEM)],
        out_specs=pl.BlockSpec(memory_space=pltpu.VMEM),
        scratch_shapes=[pltpu.VMEM(x.shape, x.dtype) for x in operands]
        + [
            pltpu.SemaphoreType.DMA((len(operands),)),
            pltpu.VMEM((shards, pack_rows, TILE), F32),
            pltpu.VMEM((pack_rows, TILE), F32),
            pltpu.VMEM((1, TILE), F32),
            pltpu.VMEM((device_total, 1, TILE), F32),
            pltpu.VMEM((3, 6 * FEATURES, nodes), BF16),
            pltpu.VMEM((clusters, leaves), BF16),
            pltpu.VMEM((2, device_total, nodes), BF16),
            pltpu.VMEM((TILE, TILE), F32),
            pltpu.VMEM((TILE, device_total), F32),
            pltpu.VMEM((source_tiles, 3, nodes), F32),
            pltpu.SemaphoreType.DMA,
            pltpu.SemaphoreType.DMA((shards,)),
            pltpu.SemaphoreType.DMA,
            pltpu.SemaphoreType.DMA,
            pltpu.SemaphoreType.DMA,
            pltpu.SemaphoreType.DMA((groups,)),
        ],
        compiler_params=pltpu.CompilerParams(collective_id=0, has_side_effects=True),
    )(*operands, block_count)
    return leaf_emit + leaf_albedo * gathered


def body(groups, shards, *args):
    leaves, nodes, slots = args[3].shape[0], args[5].shape[1], args[7].shape[1]
    per_shard = (nodes - leaves) // TILE
    source_tiles = shards * per_shard
    dense = (
        nodes // TILE * source_tiles <= TILE
        and TILE % source_tiles == 0
        and source_tiles % 8 == 0
        and nodes % (2 * TILE) == 0
        and nodes % shards == 0
        and nodes // shards <= TILE
        and shards & (shards - 1) == 0
        and shards % 2 == 0
        and groups & (groups - 1) == 0
        and groups * shards <= TILE
        and slots == TILE
    )
    return dense_body(groups, shards, *args) if dense else listed_body(*args)


def solution(mesh):
    in_specs = (
        P(None, "dev"),
        P(None, "dev"),
        P(None, "dev"),
        P("dev"),
        P("dev"),
        P(None, "dev"),
        P(None, "dev"),
        P("grp", "dev"),
        P("grp", "dev"),
        P("grp", "dev"),
    )
    out_specs = P(None, "dev")
    sized = functools.partial(body, mesh.shape["grp"], mesh.shape["dev"])
    return jax.shard_map(sized, mesh=mesh, in_specs=in_specs, out_specs=out_specs, check_vma=False)
```

```python
import functools
import jax
import jax.numpy as jnp
from jax import lax
from jax.experimental import pallas as pl
from jax.experimental.pallas import tpu as pltpu
from jax.sharding import PartitionSpec as P

TILE = 128


batch_slots = 16


def unit_normals(node_angles):
    azimuth = node_angles[0]
    elevation = node_angles[1]
    return jnp.stack(
        [
            jnp.cos(azimuth) * jnp.cos(elevation),
            jnp.sin(azimuth) * jnp.cos(elevation),
            jnp.sin(elevation),
        ]
    )


def tile_irradiance(receivers, sources):
    offsets = [
        sources[axis_id][:, None, :] - receivers[axis_id][:, :, None] for axis_id in range(3)
    ]
    distance_sq = offsets[0] * offsets[0] + offsets[1] * offsets[1] + offsets[2] * offsets[2]
    facing_receiver = (
        receivers[3][:, :, None] * offsets[0]
        + receivers[4][:, :, None] * offsets[1]
        + receivers[5][:, :, None] * offsets[2]
    )
    facing_source = (
        sources[3][:, None, :] * offsets[0]
        + sources[4][:, None, :] * offsets[1]
        + sources[5][:, None, :] * offsets[2]
    )
    source_area = sources[6][:, None, :]
    factor = (
        source_area
        * jnp.maximum(facing_receiver, 0.0)
        * jnp.maximum(-facing_source, 0.0)
        / ((distance_sq + source_area) * (jnp.pi * distance_sq + source_area))
    )
    return jnp.einsum("bij,cbj->bci", factor, sources[7:10], precision=lax.Precision.HIGHEST)


def listed_body(
    leaf_emit,
    leaf_albedo,
    leaf_radiosity,
    leaf_area,
    parent_index,
    node_position,
    node_angles,
    block_receiver,
    block_source,
    block_count,
):
    leaf_count = leaf_area.shape[0]
    node_count = node_position.shape[1]
    cluster_count = node_count - leaf_count
    tile_count = node_count // TILE
    slot_count = block_receiver.shape[1]
    normals = unit_normals(node_angles)
    parent_onehot = (
        parent_index[:, None] == jnp.arange(cluster_count, dtype=jnp.int32)[None, :]
    ).astype(jnp.float32)
    cluster_area = jnp.dot(leaf_area, parent_onehot, precision=lax.Precision.HIGHEST)
    weighted = jnp.dot(
        leaf_radiosity * leaf_area[None, :], parent_onehot, precision=lax.Precision.HIGHEST
    )
    cluster_radiosity = weighted / cluster_area[None, :]
    source_pack = jnp.concatenate(
        [
            node_position[:, leaf_count:],
            normals[:, leaf_count:],
            cluster_area[None, :],
            cluster_radiosity,
        ],
        axis=0,
    )
    receiver_pack = jnp.concatenate([node_position, normals], axis=0)
    linked = lax.all_to_all(receiver_pack, "dev", split_axis=1, concat_axis=1, tiled=True)
    receiver_tiles = linked.reshape(6, tile_count, TILE)
    everything = lax.all_gather(source_pack, "dev", axis=1, tiled=True)
    source_tiles = everything.reshape(10, -1, TILE)
    receiver_ids = block_receiver[0]
    source_ids = block_source[0]
    live_count = block_count[0, 0]
    step_slots = min(batch_slots, slot_count)

    def add_batch(rounds, totals):
        first = rounds * step_slots
        batch_receivers = lax.dynamic_slice_in_dim(receiver_ids, first, step_slots, 0)
        batch_sources = lax.dynamic_slice_in_dim(source_ids, first, step_slots, 0)
        batch_weight = (first + jnp.arange(step_slots, dtype=jnp.int32) < live_count).astype(
            jnp.float32
        )
        receivers = jnp.take(receiver_tiles, batch_receivers, axis=1)
        sources = jnp.take(source_tiles, batch_sources, axis=1)
        contrib = tile_irradiance(receivers, sources) * batch_weight[:, None, None]
        placement = (
            batch_receivers[:, None] == jnp.arange(tile_count, dtype=jnp.int32)[None, :]
        ).astype(jnp.float32)
        return totals + jnp.einsum(
            "bt,bci->cti", placement, contrib, precision=lax.Precision.HIGHEST
        )

    batch_total = (live_count + step_slots - 1) // step_slots
    totals = lax.fori_loop(0, batch_total, add_batch, jnp.zeros((3, tile_count, TILE), jnp.float32))
    partial_value = totals.reshape(3, node_count)
    summed = lax.psum(partial_value, "grp")
    irradiance = lax.all_to_all(summed, "dev", split_axis=1, concat_axis=1, tiled=True)
    pushed = jnp.dot(irradiance[:, leaf_count:], parent_onehot.T, precision=lax.Precision.HIGHEST)
    gathered = irradiance[:, :leaf_count] + pushed
    return leaf_emit + leaf_albedo * gathered


F32 = jnp.float32
BF16 = jnp.bfloat16
MESH = pl.DeviceIdType.MESH
NT_DIMS = (((1,), (1,)), ((), ()))
FEATURES = 8
RELAY_TURN = 4
HELD_PAIRS = 1
ROWS = 64


def split3(values):
    high = values.astype(BF16).astype(F32)
    rest = values - high
    middle = rest.astype(BF16).astype(F32)
    return high, middle, rest - middle


def stack3(values):
    rows = values.shape[0]
    pad = jnp.zeros((16 - 3 * rows, values.shape[1]), F32)
    return jnp.concatenate(list(split3(values)) + [pad], axis=0).astype(BF16)


def unstack3(product, rows):
    return product[0:rows] + product[rows : 2 * rows] + product[2 * rows : 3 * rows]


def flip(k, turn, shards):
    value, bit = 0, 1
    while bit < shards:
        digit = k // bit % 2
        value = value + bit * ((1 - digit) if turn // bit % 2 else digit)
        bit *= 2
    return value


def all_bits(g, pattern, groups, wanted):
    value, bit = 1, 1
    while bit < groups:
        if pattern // bit % 2:
            digit = g // bit % 2
            value = value * (digit if wanted else 1 - digit)
        bit *= 2
    return value


def paired_rows(left, const):
    one, two, three = split3(left)
    row = lax.broadcasted_iota(jnp.int32, left.shape, 0)
    free = (row == 6) | (row == 7)
    plain = [jnp.where(free, 0.0, part) for part in (one, two, three)]
    zero = jnp.zeros_like(left)
    c1, c2, c3 = [zero] * 3 if const is None else split3(jnp.broadcast_to(const, left.shape))
    at6 = row == 6
    with_sum = jnp.where(free, left, one)
    return jnp.concatenate(
        [
            with_sum,
            jnp.where(at6, c1, plain[1]),
            jnp.where(at6, c2, plain[2]),
            with_sum,
            jnp.where(at6, c3, plain[1]),
            with_sum,
        ],
        axis=0,
    ).astype(BF16)


def dense_kernel(groups, shards, *refs):
    operands, count, out, inputs, scratch = refs[:7], refs[7], refs[8], refs[9:16], refs[16:]
    receiver_id, source_id, area, parent, angles, radiosity, position = inputs
    (
        load,
        sources, my_pack, my_hist, hists, right, onehot, place, columns, turned, sums,
        src_send, src_recv, hist_send, hist_recv, pass_send, peer_recv,
    ) = scratch
    g = lax.axis_index("grp")
    k = lax.axis_index("dev")
    device_total = groups * shards
    me = g * shards + k
    leaves = radiosity.shape[1]
    nodes = position.shape[1]
    clusters = nodes - leaves
    per_shard = clusters // TILE
    source_tiles = shards * per_shard
    per_peer = nodes // shards
    chunks = nodes // TILE
    pairs = nodes // (2 * TILE)

    loads = [
        pltpu.make_async_copy(operands[i], inputs[i], load.at[max(i - 4, 0)])
        for i in range(len(inputs))
    ]
    for copy in loads:
        copy.start()

    barrier = pltpu.get_barrier_semaphore()
    group = [flip(g, e, groups) for e in range(groups)]
    drops = [all_bits(g, e, groups, True) for e in range(groups)]
    clear = [all_bits(g, e, groups, False) for e in range(groups)]

    def rows_done(rows, semaphore):
        some = hists.at[pl.ds(0, rows)]
        pltpu.make_async_copy(some, some, semaphore).wait()

    def greet(e, shard):
        pl.semaphore_signal(
            barrier, inc=1, device_id=(group[e], shard), device_id_type=MESH
        )

    def run(first, last, action):
        lax.fori_loop(first, last, lambda shard, _: (action(shard), 0)[1], 0)

    for step in range(1, shards):
        greet(0, flip(k, step, shards))
    for e in reversed(range(1, groups)):
        run(k * (1 - clear[e]), shards, lambda shard: greet(e, shard))

    rows_done(sum(x.size for x in inputs[:5]) // TILE, load.at[0])
    for copy in loads[5:]:
        copy.wait()

    lane = lax.broadcasted_iota(jnp.int32, (1, TILE), 1)
    code = jnp.where(
        lane < count[0, 0], receiver_id[...] * source_tiles + source_id[...], -1
    )
    square = lax.broadcasted_iota(jnp.int32, (TILE, TILE), 0)
    hit = jnp.where(square == code, 1.0, 0.0).astype(BF16)
    counted = lax.dot_general(
        jnp.ones((16, TILE), BF16), hit, NT_DIMS, preferred_element_type=F32
    )
    my_hist[...] = counted[0:1]
    hists[me] = counted[0:1]

    ids = lax.broadcasted_iota(jnp.int32, (clusters, leaves), 0)
    onehot[...] = jnp.where(ids == parent[...], 1.0, 0.0).astype(BF16)
    area_row = area[...]
    stacked = stack3(jnp.concatenate([area_row, radiosity[...] * area_row], axis=0))
    cluster = unstack3(
        lax.dot_general(stacked, onehot[...], NT_DIMS, preferred_element_type=F32), 4
    )
    cosines = jnp.cos(angles[...])
    sines = jnp.sin(angles[...])
    normals = jnp.concatenate(
        [cosines[0:1] * cosines[1:2], sines[0:1] * cosines[1:2], sines[1:2]], axis=0
    )
    first_band = cluster[1:2] * (1.0 / jnp.pi)
    facing = normals[:, leaves:] * first_band
    ratios = cluster[2:4] / cluster[1:2]
    for half in range(per_shard):
        here = slice(half * TILE, (half + 1) * TILE)
        there = slice(leaves + half * TILE, leaves + (half + 1) * TILE)
        my_pack[8 * half : 8 * half + 8, :] = jnp.concatenate(
            [position[:, there], facing[:, here], cluster[0:1, here], ratios[0:1, here]], axis=0
        )
        my_pack[8 * per_shard + half : 8 * per_shard + half + 1, :] = ratios[1:2, here]

    drop_total = sum(drops[1:], 1)
    pl.semaphore_wait(barrier, groups - 1 + groups * k + (shards - 1 - k) * drop_total)

    def hist_copy(e, shard):
        return pltpu.make_async_remote_copy(
            src_ref=my_hist,
            dst_ref=hists.at[me],
            send_sem=hist_send,
            recv_sem=hist_recv,
            device_id=(group[e], shard),
            device_id_type=MESH,
        )

    def peer_copy(e):
        return pltpu.make_async_remote_copy(
            src_ref=my_hist,
            dst_ref=hists.at[me],
            send_sem=hist_send,
            recv_sem=peer_recv.at[e - 1],
            device_id=(group[e], k),
            device_id_type=MESH,
        )

    def passed_copy(e, shard):
        return pltpu.make_async_remote_copy(
            src_ref=hists.at[group[e] * shards + k],
            dst_ref=hists.at[group[e] * shards + k],
            send_sem=pass_send,
            recv_sem=hist_recv,
            device_id=(g, shard),
            device_id_type=MESH,
        )

    def source_copy(shard):
        return pltpu.make_async_remote_copy(
            src_ref=my_pack,
            dst_ref=sources.at[k],
            send_sem=src_send,
            recv_sem=src_recv.at[k // 2],
            device_id=(g, shard),
            device_id_type=MESH,
        )

    run(0, k, lambda shard: hist_copy(groups - 1, shard).start())
    run(0, k, lambda shard: source_copy(shard).start())
    run(k + 1, shards, lambda shard: source_copy(shard).start())
    for e in reversed(range(groups - 1)):
        run(0, k, lambda shard: hist_copy(e, shard).start())
    for e in range(1, groups):
        peer_copy(e).start()
    for e in range(groups):

        @pl.when(drops[e] == 1)
        def _():
            run(k + 1, shards, lambda shard: hist_copy(e, shard).start())

    middle = jnp.sum(position[...], axis=1, keepdims=True) * (1.0 / nodes)
    centred = position[...] - middle
    ones = jnp.ones((1, nodes), F32)
    none = jnp.zeros((1, nodes), F32)
    three = jnp.zeros((3, nodes), F32)
    offset = -jnp.sum(normals * centred, axis=0, keepdims=True)
    norm = jnp.sum(centred * centred, axis=0, keepdims=True)
    for which, rows in enumerate(
        (
            paired_rows(jnp.concatenate([normals, three, none, none], axis=0), offset),
            paired_rows(jnp.concatenate([three, centred, -ones, none], axis=0), None),
            paired_rows(jnp.concatenate([-2.0 * centred, three, none, ones], axis=0), norm),
        )
    ):
        right[which] = rows

    node = lax.broadcasted_iota(jnp.int32, (1, nodes), 1)
    link = jnp.zeros((1, nodes), jnp.int32)
    for j in range(1, shards):
        link += jnp.where(node >= j * per_peer, 1, 0)
    spot = k * per_peer + node - link * per_peer
    low_tile = k * per_peer // TILE
    high_tile = (k * per_peer + per_peer - 1) // TILE
    upper = spot >= (low_tile + 1) * TILE
    owner_row = lax.broadcasted_iota(jnp.int32, (device_total, nodes), 0) % shards
    hits = owner_row == link
    place[0] = jnp.where(hits & ~upper, 1.0, 0.0).astype(BF16)
    place[1] = jnp.where(hits & upper, 1.0, 0.0).astype(BF16)

    row8 = lax.broadcasted_iota(jnp.int32, (8, TILE), 0)
    centre8 = jnp.concatenate([middle, jnp.zeros((5, 1), F32)], axis=0)

    def prepare(pack, half, tile):
        values = pack[8 * half : 8 * half + 8, :]
        ratio = pack[8 * per_shard + half : 8 * per_shard + half + 1, :]
        area_here = values[6:7]
        shifted = values - centre8
        spots, aims = shifted[0:3], shifted[3:6]
        along = jnp.sum(spots * aims, axis=0, keepdims=True)
        reach = jnp.sum(spots * spots, axis=0, keepdims=True) + area_here
        one, two, low = split3(jnp.concatenate([spots, aims, along, reach], axis=0))
        left = jnp.concatenate(
            [
                one,
                jnp.where(row8 == 6, 1.0, one),
                jnp.where(row8 == 6, 1.0, one),
                two,
                jnp.where(row8 == 6, 1.0, two),
                low,
            ],
            axis=0,
        )
        extra = jnp.concatenate(
            [values[7:8], ratio, area_here * ((jnp.pi - 1.0) / jnp.pi), jnp.zeros((5, TILE), F32)],
            axis=0,
        )
        features = jnp.transpose(left).astype(BF16)
        column = jnp.transpose(extra)
        second, third, less = [
            jnp.broadcast_to(column[:, i : i + 1], (TILE, TILE)) for i in range(3)
        ]
        return features, second, third, less, tile

    def products(features, pair):
        wide = slice(pair * 2 * TILE, (pair + 1) * 2 * TILE)
        return [
            [
                jnp.dot(
                    features[first : first + ROWS], right[which, :, wide],
                    preferred_element_type=F32,
                )
                for which in range(3)
            ]
            for first in range(0, TILE, ROWS)
        ]

    def finish(parts, pair, second, third, less, tile):
        totals = [[None] * 3, [None] * 3]
        for first, (toward, facing, span) in zip(range(0, TILE, ROWS), parts):
            some = slice(first, first + ROWS)
            for side in range(2):
                lanes = slice(side * TILE, (side + 1) * TILE)
                u = span[:, lanes]
                form = (
                    jnp.maximum(toward[:, lanes], 0.0)
                    * jnp.maximum(facing[:, lanes], 0.0)
                    / (u * (u - less[some]))
                )
                for c, scaled in enumerate((form, form * second[some], form * third[some])):
                    part = jnp.sum(scaled.reshape(ROWS // 8, 8, TILE), axis=0)
                    old = totals[side][c]
                    totals[side][c] = part if old is None else old + part
        for side in range(2):
            first = pair * 2 * TILE + side * TILE
            for c in range(3):
                sums[tile, c, :, first : first + TILE] = totals[side][c]

    def settle():
        everything = sources.at[pl.ds(0, shards - 1)]
        pltpu.make_async_copy(everything, everything, src_send).wait()
        levels = [1]
        while levels[-1] < groups:
            levels.append(2 * levels[-1])
        for shard in range(shards):

            @pl.when(k == shard)
            def _():
                for level in levels:
                    later = shards - 1 - shard
                    rows = groups - 1 + groups * shard + later * level
                    passed = later * (groups - groups // level)

                    @pl.when(drop_total == level)
                    def _():
                        rows_done(rows, hist_send)
                        if passed:
                            rows_done(passed, pass_send)

    def peer_arrival(e):
        pltpu.make_async_remote_copy(
            src_ref=my_hist,
            dst_ref=hists.at[group[e] * shards + k],
            send_sem=hist_send,
            recv_sem=peer_recv.at[e - 1],
            device_id=(group[e], k),
            device_id_type=MESH,
        ).wait_recv()

    held = []
    for first in range(0, shards, 2):
        if first == RELAY_TURN:
            for e in range(1, groups):

                @pl.when(clear[e] == 0)
                def _():
                    peer_arrival(e)
                    run(k + 1, shards, lambda shard: passed_copy(e, shard).start())

        if first == shards - 2:
            settle()
        owners = [flip(k, first, shards), flip(k, first + 1, shards)]
        if first:
            both = sources.at[pl.ds(owners[0] // 2 * 2, 2)]
        else:
            both = sources.at[owners[1]]
        pltpu.make_async_copy(both, both, src_recv.at[owners[0] // 2]).wait()
        packs = [(sources.at[owner], owner) for owner in owners]
        if not first:
            packs[0] = (my_pack, k)
        ready = [
            prepare(pack, half, owner * per_shard + half)
            for pack, owner in packs
            for half in range(per_shard)
        ]
        for work in held:
            finish(*work)
        held = []
        for number, (features, *rest) in enumerate(ready):
            for pair in range(pairs):
                work = (products(features, pair), pair, *rest)
                if number == len(ready) - 1 and pair >= pairs - HELD_PAIRS:
                    held.append(work)
                else:
                    finish(*work)

    for e in range(1, groups):

        @pl.when(clear[e] == 1)
        def _():
            peer_arrival(e)

    distant = hists.at[pl.ds(0, groups * (shards - 1))]
    pltpu.make_async_copy(distant, distant, hist_recv).wait()
    table = jnp.concatenate([hists[d] for d in range(device_total)], axis=0)
    turned[...] = jnp.transpose(table)
    weight = jnp.zeros((source_tiles, nodes), F32)
    for which, tile in enumerate((low_tile, high_tile)):
        rows = turned[pl.ds(pl.multiple_of(tile * source_tiles, 8), source_tiles), :]
        weight += jnp.dot(rows.astype(BF16), place[which], preferred_element_type=F32)
    for work in held:
        finish(*work)

    chunk_rows = []
    for chunk in range(chunks):
        lanes = slice(chunk * TILE, (chunk + 1) * TILE)
        totals = [None] * 3
        for tile in range(source_tiles):
            scale = jnp.broadcast_to(weight[tile : tile + 1, lanes], (8, TILE))
            for c in range(3):
                part = scale * sums[tile, c, :, lanes]
                totals[c] = part if totals[c] is None else totals[c] + part
        chunk_rows.append(
            jnp.concatenate([jnp.sum(x, axis=0, keepdims=True) for x in totals], axis=0)
        )
    irradiance = jnp.concatenate(chunk_rows, axis=1)
    pushed = unstack3(
        jnp.dot(stack3(irradiance[:, leaves:]), onehot[...], preferred_element_type=F32), 3
    )
    out[...] = irradiance[:, :leaves] + pushed


def dense_body(
    groups, shards, leaf_emit, leaf_albedo, leaf_radiosity, leaf_area, parent_index,
    node_position, node_angles, block_receiver, block_source, block_count,
):
    leaves = leaf_area.shape[0]
    nodes = node_position.shape[1]
    clusters = nodes - leaves
    per_shard = clusters // TILE
    source_tiles = shards * per_shard
    device_total = groups * shards
    operands = (
        block_receiver, block_source, leaf_area[None, :], parent_index[None, :], node_angles,
        leaf_radiosity, node_position,
    )
    pack_rows = 9 * per_shard
    gathered = pl.pallas_call(
        functools.partial(dense_kernel, groups, shards),
        out_shape=pltpu.VMEM((3, leaves), F32),
        in_specs=[pl.BlockSpec(memory_space=pltpu.HBM)] * len(operands)
        + [pl.BlockSpec(memory_space=pltpu.SMEM)],
        out_specs=pl.BlockSpec(memory_space=pltpu.VMEM),
        scratch_shapes=[pltpu.VMEM(x.shape, x.dtype) for x in operands]
        + [
            pltpu.SemaphoreType.DMA((len(operands) - 4,)),
            pltpu.VMEM((shards, pack_rows, TILE), F32),
            pltpu.VMEM((pack_rows, TILE), F32),
            pltpu.VMEM((1, TILE), F32),
            pltpu.VMEM((device_total, 1, TILE), F32),
            pltpu.VMEM((3, 6 * FEATURES, nodes), BF16),
            pltpu.VMEM((clusters, leaves), BF16),
            pltpu.VMEM((2, device_total, nodes), BF16),
            pltpu.VMEM((TILE, TILE), F32),
            pltpu.VMEM((TILE, device_total), F32),
            pltpu.VMEM((source_tiles, 3, 8, nodes), F32),
            pltpu.SemaphoreType.DMA,
            pltpu.SemaphoreType.DMA((shards // 2,)),
            pltpu.SemaphoreType.DMA,
            pltpu.SemaphoreType.DMA,
            pltpu.SemaphoreType.DMA,
            pltpu.SemaphoreType.DMA((groups - 1,)),
        ],
        compiler_params=pltpu.CompilerParams(collective_id=0, has_side_effects=True),
    )(*operands, block_count)
    return leaf_emit + leaf_albedo * gathered


def body(groups, shards, *args):
    leaves, nodes, slots = args[3].shape[0], args[5].shape[1], args[7].shape[1]
    per_shard = (nodes - leaves) // TILE
    source_tiles = shards * per_shard
    dense = (
        nodes // TILE * source_tiles <= TILE
        and TILE % source_tiles == 0
        and source_tiles % 8 == 0
        and nodes % (2 * TILE) == 0
        and leaves % TILE == 0
        and groups > 1
        and nodes % shards == 0
        and nodes // shards <= TILE
        and shards & (shards - 1) == 0
        and shards % 2 == 0
        and groups & (groups - 1) == 0
        and groups * shards <= TILE
        and slots == TILE
    )
    return dense_body(groups, shards, *args) if dense else listed_body(*args)


def solution(mesh):
    in_specs = (
        P(None, "dev"),
        P(None, "dev"),
        P(None, "dev"),
        P("dev"),
        P("dev"),
        P(None, "dev"),
        P(None, "dev"),
        P("grp", "dev"),
        P("grp", "dev"),
        P("grp", "dev"),
    )
    out_specs = P(None, "dev")
    sized = functools.partial(body, mesh.shape["grp"], mesh.shape["dev"])
    return jax.shard_map(sized, mesh=mesh, in_specs=in_specs, out_specs=out_specs, check_vma=False)
```

```python
import functools
import jax
import jax.numpy as jnp
from jax import lax
from jax.experimental import pallas as pl
from jax.experimental.pallas import tpu as pltpu
from jax.sharding import PartitionSpec as P

TILE = 128


batch_slots = 16


def unit_normals(node_angles):
    azimuth = node_angles[0]
    elevation = node_angles[1]
    return jnp.stack(
        [
            jnp.cos(azimuth) * jnp.cos(elevation),
            jnp.sin(azimuth) * jnp.cos(elevation),
            jnp.sin(elevation),
        ]
    )


def tile_irradiance(receivers, sources):
    offsets = [
        sources[axis_id][:, None, :] - receivers[axis_id][:, :, None] for axis_id in range(3)
    ]
    distance_sq = offsets[0] * offsets[0] + offsets[1] * offsets[1] + offsets[2] * offsets[2]
    facing_receiver = (
        receivers[3][:, :, None] * offsets[0]
        + receivers[4][:, :, None] * offsets[1]
        + receivers[5][:, :, None] * offsets[2]
    )
    facing_source = (
        sources[3][:, None, :] * offsets[0]
        + sources[4][:, None, :] * offsets[1]
        + sources[5][:, None, :] * offsets[2]
    )
    source_area = sources[6][:, None, :]
    factor = (
        source_area
        * jnp.maximum(facing_receiver, 0.0)
        * jnp.maximum(-facing_source, 0.0)
        / ((distance_sq + source_area) * (jnp.pi * distance_sq + source_area))
    )
    return jnp.einsum("bij,cbj->bci", factor, sources[7:10], precision=lax.Precision.HIGHEST)


def listed_body(
    leaf_emit,
    leaf_albedo,
    leaf_radiosity,
    leaf_area,
    parent_index,
    node_position,
    node_angles,
    block_receiver,
    block_source,
    block_count,
):
    leaf_count = leaf_area.shape[0]
    node_count = node_position.shape[1]
    cluster_count = node_count - leaf_count
    tile_count = node_count // TILE
    slot_count = block_receiver.shape[1]
    normals = unit_normals(node_angles)
    parent_onehot = (
        parent_index[:, None] == jnp.arange(cluster_count, dtype=jnp.int32)[None, :]
    ).astype(jnp.float32)
    cluster_area = jnp.dot(leaf_area, parent_onehot, precision=lax.Precision.HIGHEST)
    weighted = jnp.dot(
        leaf_radiosity * leaf_area[None, :], parent_onehot, precision=lax.Precision.HIGHEST
    )
    cluster_radiosity = weighted / cluster_area[None, :]
    source_pack = jnp.concatenate(
        [
            node_position[:, leaf_count:],
            normals[:, leaf_count:],
            cluster_area[None, :],
            cluster_radiosity,
        ],
        axis=0,
    )
    receiver_pack = jnp.concatenate([node_position, normals], axis=0)
    linked = lax.all_to_all(receiver_pack, "dev", split_axis=1, concat_axis=1, tiled=True)
    receiver_tiles = linked.reshape(6, tile_count, TILE)
    everything = lax.all_gather(source_pack, "dev", axis=1, tiled=True)
    source_tiles = everything.reshape(10, -1, TILE)
    receiver_ids = block_receiver[0]
    source_ids = block_source[0]
    live_count = block_count[0, 0]
    step_slots = min(batch_slots, slot_count)

    def add_batch(rounds, totals):
        first = rounds * step_slots
        batch_receivers = lax.dynamic_slice_in_dim(receiver_ids, first, step_slots, 0)
        batch_sources = lax.dynamic_slice_in_dim(source_ids, first, step_slots, 0)
        batch_weight = (first + jnp.arange(step_slots, dtype=jnp.int32) < live_count).astype(
            jnp.float32
        )
        receivers = jnp.take(receiver_tiles, batch_receivers, axis=1)
        sources = jnp.take(source_tiles, batch_sources, axis=1)
        contrib = tile_irradiance(receivers, sources) * batch_weight[:, None, None]
        placement = (
            batch_receivers[:, None] == jnp.arange(tile_count, dtype=jnp.int32)[None, :]
        ).astype(jnp.float32)
        return totals + jnp.einsum(
            "bt,bci->cti", placement, contrib, precision=lax.Precision.HIGHEST
        )

    batch_total = (live_count + step_slots - 1) // step_slots
    totals = lax.fori_loop(0, batch_total, add_batch, jnp.zeros((3, tile_count, TILE), jnp.float32))
    partial_value = totals.reshape(3, node_count)
    summed = lax.psum(partial_value, "grp")
    irradiance = lax.all_to_all(summed, "dev", split_axis=1, concat_axis=1, tiled=True)
    pushed = jnp.dot(irradiance[:, leaf_count:], parent_onehot.T, precision=lax.Precision.HIGHEST)
    gathered = irradiance[:, :leaf_count] + pushed
    return leaf_emit + leaf_albedo * gathered


F32 = jnp.float32
BF16 = jnp.bfloat16
MESH = pl.DeviceIdType.MESH
NT_DIMS = (((1,), (1,)), ((), ()))
FEATURES = 8
RELAY_TURN = 4
HELD_PAIRS = 1
ROWS = 64


def split3(values):
    high = values.astype(BF16).astype(F32)
    rest = values - high
    middle = rest.astype(BF16).astype(F32)
    return high, middle, rest - middle


def stack3(values):
    rows = values.shape[0]
    pad = jnp.zeros((16 - 3 * rows, values.shape[1]), F32)
    return jnp.concatenate(list(split3(values)) + [pad], axis=0).astype(BF16)


def unstack3(product, rows):
    return product[0:rows] + product[rows : 2 * rows] + product[2 * rows : 3 * rows]


def flip(k, turn, shards):
    value, bit = 0, 1
    while bit < shards:
        digit = k // bit % 2
        value = value + bit * ((1 - digit) if turn // bit % 2 else digit)
        bit *= 2
    return value


def all_bits(g, pattern, groups, wanted):
    value, bit = 1, 1
    while bit < groups:
        if pattern // bit % 2:
            digit = g // bit % 2
            value = value * (digit if wanted else 1 - digit)
        bit *= 2
    return value


def paired_rows(left, const):
    one, two, three = split3(left)
    row = lax.broadcasted_iota(jnp.int32, left.shape, 0)
    free = (row == 6) | (row == 7)
    plain = [jnp.where(free, 0.0, part) for part in (one, two, three)]
    zero = jnp.zeros_like(left)
    c1, c2, c3 = [zero] * 3 if const is None else split3(jnp.broadcast_to(const, left.shape))
    at6 = row == 6
    with_sum = jnp.where(free, left, one)
    return jnp.concatenate(
        [
            with_sum,
            jnp.where(at6, c1, plain[1]),
            jnp.where(at6, c2, plain[2]),
            with_sum,
            jnp.where(at6, c3, plain[1]),
            with_sum,
        ],
        axis=0,
    ).astype(BF16)


def dense_kernel(groups, shards, *refs):
    operands, count, out, inputs, scratch = refs[:7], refs[7], refs[8], refs[9:16], refs[16:]
    receiver_id, source_id, area, parent, angles, radiosity, position = inputs
    (
        load,
        sources, my_pack, my_hist, hists, right, onehot, place, columns, turned, sums,
        src_send, src_recv, hist_send, hist_recv, pass_send, peer_recv,
    ) = scratch
    g = lax.axis_index("grp")
    k = lax.axis_index("dev")
    device_total = groups * shards
    me = g * shards + k
    leaves = radiosity.shape[1]
    nodes = position.shape[1]
    clusters = nodes - leaves
    per_shard = clusters // TILE
    source_tiles = shards * per_shard
    per_peer = nodes // shards
    chunks = nodes // TILE
    pairs = nodes // (2 * TILE)

    loads = [
        pltpu.make_async_copy(operands[i], inputs[i], load.at[max(i - 4, 0)])
        for i in range(len(inputs))
    ]
    for copy in loads:
        copy.start()

    barrier = pltpu.get_barrier_semaphore()
    group = [flip(g, e, groups) for e in range(groups)]
    drops = [all_bits(g, e, groups, True) for e in range(groups)]
    clear = [all_bits(g, e, groups, False) for e in range(groups)]

    def rows_done(rows, semaphore):
        some = hists.at[pl.ds(0, rows)]
        pltpu.make_async_copy(some, some, semaphore).wait()

    def greet(e, shard):
        pl.semaphore_signal(
            barrier, inc=1, device_id=(group[e], shard), device_id_type=MESH
        )

    def run(first, last, action):
        lax.fori_loop(first, last, lambda shard, _: (action(shard), 0)[1], 0)

    for step in range(1, shards):
        greet(0, flip(k, step, shards))
    for e in reversed(range(1, groups)):
        run(k * (1 - clear[e]), shards, lambda shard: greet(e, shard))

    rows_done(sum(x.size for x in inputs[:5]) // TILE, load.at[0])
    for copy in loads[5:]:
        copy.wait()

    lane = lax.broadcasted_iota(jnp.int32, (1, TILE), 1)
    code = jnp.where(
        lane < count[0, 0], receiver_id[...] * source_tiles + source_id[...], -1
    )
    square = lax.broadcasted_iota(jnp.int32, (TILE, TILE), 0)
    hit = jnp.where(square == code, 1.0, 0.0).astype(BF16)
    counted = lax.dot_general(
        jnp.ones((16, TILE), BF16), hit, NT_DIMS, preferred_element_type=F32
    )
    my_hist[...] = counted[0:1]
    hists[me] = counted[0:1]

    ids = lax.broadcasted_iota(jnp.int32, (clusters, leaves), 0)
    onehot[...] = jnp.where(ids == parent[...], 1.0, 0.0).astype(BF16)
    area_row = area[...]
    stacked = stack3(jnp.concatenate([area_row, radiosity[...] * area_row], axis=0))
    cluster = unstack3(
        lax.dot_general(stacked, onehot[...], NT_DIMS, preferred_element_type=F32), 4
    )
    cosines = jnp.cos(angles[...])
    sines = jnp.sin(angles[...])
    normals = jnp.concatenate(
        [cosines[0:1] * cosines[1:2], sines[0:1] * cosines[1:2], sines[1:2]], axis=0
    )
    first_band = cluster[1:2] * (1.0 / jnp.pi)
    facing = normals[:, leaves:] * first_band
    ratios = cluster[2:4] / cluster[1:2]
    for half in range(per_shard):
        here = slice(half * TILE, (half + 1) * TILE)
        there = slice(leaves + half * TILE, leaves + (half + 1) * TILE)
        my_pack[8 * half : 8 * half + 8, :] = jnp.concatenate(
            [position[:, there], facing[:, here], cluster[0:1, here], ratios[0:1, here]], axis=0
        )
        my_pack[8 * per_shard + half : 8 * per_shard + half + 1, :] = ratios[1:2, here]

    drop_total = sum(drops[1:], 1)
    pl.semaphore_wait(barrier, groups - 1 + groups * k + (shards - 1 - k) * drop_total)

    def hist_copy(e, shard):
        return pltpu.make_async_remote_copy(
            src_ref=my_hist,
            dst_ref=hists.at[me],
            send_sem=hist_send,
            recv_sem=hist_recv,
            device_id=(group[e], shard),
            device_id_type=MESH,
        )

    def peer_copy(e):
        return pltpu.make_async_remote_copy(
            src_ref=my_hist,
            dst_ref=hists.at[me],
            send_sem=hist_send,
            recv_sem=peer_recv.at[e - 1],
            device_id=(group[e], k),
            device_id_type=MESH,
        )

    def passed_copy(e, shard):
        return pltpu.make_async_remote_copy(
            src_ref=hists.at[group[e] * shards + k],
            dst_ref=hists.at[group[e] * shards + k],
            send_sem=pass_send,
            recv_sem=hist_recv,
            device_id=(g, shard),
            device_id_type=MESH,
        )

    def source_copy(shard):
        return pltpu.make_async_remote_copy(
            src_ref=my_pack,
            dst_ref=sources.at[k],
            send_sem=src_send,
            recv_sem=src_recv.at[k // 2],
            device_id=(g, shard),
            device_id_type=MESH,
        )

    urgent = jnp.minimum(k, 2)
    run(0, urgent, lambda shard: hist_copy(groups - 1, shard).start())
    run(0, k, lambda shard: source_copy(shard).start())
    run(k + 1, shards, lambda shard: source_copy(shard).start())
    run(urgent, k, lambda shard: hist_copy(groups - 1, shard).start())
    for e in reversed(range(groups - 1)):
        run(0, k, lambda shard: hist_copy(e, shard).start())
    for e in range(1, groups):
        peer_copy(e).start()
    for e in range(groups):

        @pl.when(drops[e] == 1)
        def _():
            run(k + 1, shards, lambda shard: hist_copy(e, shard).start())

    middle = jnp.sum(position[...], axis=1, keepdims=True) * (1.0 / nodes)
    centred = position[...] - middle
    ones = jnp.ones((1, nodes), F32)
    none = jnp.zeros((1, nodes), F32)
    three = jnp.zeros((3, nodes), F32)
    offset = -jnp.sum(normals * centred, axis=0, keepdims=True)
    norm = jnp.sum(centred * centred, axis=0, keepdims=True)
    for which, rows in enumerate(
        (
            paired_rows(jnp.concatenate([normals, three, none, none], axis=0), offset),
            paired_rows(jnp.concatenate([three, centred, -ones, none], axis=0), None),
            paired_rows(jnp.concatenate([-2.0 * centred, three, none, ones], axis=0), norm),
        )
    ):
        right[which] = rows

    node = lax.broadcasted_iota(jnp.int32, (1, nodes), 1)
    link = jnp.zeros((1, nodes), jnp.int32)
    for j in range(1, shards):
        link += jnp.where(node >= j * per_peer, 1, 0)
    spot = k * per_peer + node - link * per_peer
    low_tile = k * per_peer // TILE
    high_tile = (k * per_peer + per_peer - 1) // TILE
    upper = spot >= (low_tile + 1) * TILE
    owner_row = lax.broadcasted_iota(jnp.int32, (device_total, nodes), 0) % shards
    hits = owner_row == link
    place[0] = jnp.where(hits & ~upper, 1.0, 0.0).astype(BF16)
    place[1] = jnp.where(hits & upper, 1.0, 0.0).astype(BF16)

    row8 = lax.broadcasted_iota(jnp.int32, (8, TILE), 0)
    centre8 = jnp.concatenate([middle, jnp.zeros((5, 1), F32)], axis=0)

    def prepare(pack, half, tile):
        values = pack[8 * half : 8 * half + 8, :]
        ratio = pack[8 * per_shard + half : 8 * per_shard + half + 1, :]
        area_here = values[6:7]
        shifted = values - centre8
        spots, aims = shifted[0:3], shifted[3:6]
        along = jnp.sum(spots * aims, axis=0, keepdims=True)
        reach = jnp.sum(spots * spots, axis=0, keepdims=True) + area_here
        one, two, low = split3(jnp.concatenate([spots, aims, along, reach], axis=0))
        left = jnp.concatenate(
            [
                one,
                jnp.where(row8 == 6, 1.0, one),
                jnp.where(row8 == 6, 1.0, one),
                two,
                jnp.where(row8 == 6, 1.0, two),
                low,
            ],
            axis=0,
        )
        extra = jnp.concatenate(
            [values[7:8], ratio, area_here * ((jnp.pi - 1.0) / jnp.pi), jnp.zeros((5, TILE), F32)],
            axis=0,
        )
        features = jnp.transpose(left).astype(BF16)
        column = jnp.transpose(extra)
        second, third, less = [
            jnp.broadcast_to(column[:, i : i + 1], (TILE, TILE)) for i in range(3)
        ]
        return features, second, third, less, tile

    def products(features, pair):
        wide = slice(pair * 2 * TILE, (pair + 1) * 2 * TILE)
        return [
            [
                jnp.dot(
                    features[first : first + ROWS], right[which, :, wide],
                    preferred_element_type=F32,
                )
                for which in range(3)
            ]
            for first in range(0, TILE, ROWS)
        ]

    def finish(parts, pair, second, third, less, tile):
        totals = [[None] * 3, [None] * 3]
        for first, (toward, facing, span) in zip(range(0, TILE, ROWS), parts):
            some = slice(first, first + ROWS)
            for side in range(2):
                lanes = slice(side * TILE, (side + 1) * TILE)
                u = span[:, lanes]
                form = (
                    jnp.maximum(toward[:, lanes], 0.0)
                    * jnp.maximum(facing[:, lanes], 0.0)
                    / (u * (u - less[some]))
                )
                for c, scaled in enumerate((form, form * second[some], form * third[some])):
                    part = jnp.sum(scaled.reshape(ROWS // 8, 8, TILE), axis=0)
                    old = totals[side][c]
                    totals[side][c] = part if old is None else old + part
        for side in range(2):
            first = pair * 2 * TILE + side * TILE
            for c in range(3):
                sums[tile, c, :, first : first + TILE] = totals[side][c]

    def settle():
        everything = sources.at[pl.ds(0, shards - 1)]
        pltpu.make_async_copy(everything, everything, src_send).wait()
        levels = [1]
        while levels[-1] < groups:
            levels.append(2 * levels[-1])
        for shard in range(shards):

            @pl.when(k == shard)
            def _():
                for level in levels:
                    later = shards - 1 - shard
                    rows = groups - 1 + groups * shard + later * level
                    passed = later * (groups - groups // level)

                    @pl.when(drop_total == level)
                    def _():
                        rows_done(rows, hist_send)
                        if passed:
                            rows_done(passed, pass_send)

    def peer_arrival(e):
        pltpu.make_async_remote_copy(
            src_ref=my_hist,
            dst_ref=hists.at[group[e] * shards + k],
            send_sem=hist_send,
            recv_sem=peer_recv.at[e - 1],
            device_id=(group[e], k),
            device_id_type=MESH,
        ).wait_recv()

    held = []
    for first in range(0, shards, 2):
        if first == RELAY_TURN:
            for e in range(1, groups):

                @pl.when(clear[e] == 0)
                def _():
                    peer_arrival(e)
                    run(k + 1, shards, lambda shard: passed_copy(e, shard).start())

        if first == shards - 2:
            settle()
        owners = [flip(k, first, shards), flip(k, first + 1, shards)]
        if first:
            both = sources.at[pl.ds(owners[0] // 2 * 2, 2)]
        else:
            both = sources.at[owners[1]]
        pltpu.make_async_copy(both, both, src_recv.at[owners[0] // 2]).wait()
        packs = [(sources.at[owner], owner) for owner in owners]
        if not first:
            packs[0] = (my_pack, k)
        ready = [
            prepare(pack, half, owner * per_shard + half)
            for pack, owner in packs
            for half in range(per_shard)
        ]
        for work in held:
            finish(*work)
        held = []
        for number, (features, *rest) in enumerate(ready):
            for pair in range(pairs):
                work = (products(features, pair), pair, *rest)
                if number == len(ready) - 1 and pair >= pairs - HELD_PAIRS:
                    held.append(work)
                else:
                    finish(*work)

    for e in range(1, groups):

        @pl.when(clear[e] == 1)
        def _():
            peer_arrival(e)

    distant = hists.at[pl.ds(0, groups * (shards - 1))]
    pltpu.make_async_copy(distant, distant, hist_recv).wait()
    table = jnp.concatenate([hists[d] for d in range(device_total)], axis=0)
    turned[...] = jnp.transpose(table)
    weight = jnp.zeros((source_tiles, nodes), F32)
    for which, tile in enumerate((low_tile, high_tile)):
        rows = turned[pl.ds(pl.multiple_of(tile * source_tiles, 8), source_tiles), :]
        weight += jnp.dot(rows.astype(BF16), place[which], preferred_element_type=F32)
    for work in held:
        finish(*work)

    chunk_rows = []
    for chunk in range(chunks):
        lanes = slice(chunk * TILE, (chunk + 1) * TILE)
        totals = [None] * 3
        for tile in range(source_tiles):
            scale = jnp.broadcast_to(weight[tile : tile + 1, lanes], (8, TILE))
            for c in range(3):
                part = scale * sums[tile, c, :, lanes]
                totals[c] = part if totals[c] is None else totals[c] + part
        chunk_rows.append(
            jnp.concatenate([jnp.sum(x, axis=0, keepdims=True) for x in totals], axis=0)
        )
    irradiance = jnp.concatenate(chunk_rows, axis=1)
    pushed = unstack3(
        jnp.dot(stack3(irradiance[:, leaves:]), onehot[...], preferred_element_type=F32), 3
    )
    out[...] = irradiance[:, :leaves] + pushed


def dense_body(
    groups, shards, leaf_emit, leaf_albedo, leaf_radiosity, leaf_area, parent_index,
    node_position, node_angles, block_receiver, block_source, block_count,
):
    leaves = leaf_area.shape[0]
    nodes = node_position.shape[1]
    clusters = nodes - leaves
    per_shard = clusters // TILE
    source_tiles = shards * per_shard
    device_total = groups * shards
    operands = (
        block_receiver, block_source, leaf_area[None, :], parent_index[None, :], node_angles,
        leaf_radiosity, node_position,
    )
    pack_rows = 9 * per_shard
    gathered = pl.pallas_call(
        functools.partial(dense_kernel, groups, shards),
        out_shape=pltpu.VMEM((3, leaves), F32),
        in_specs=[pl.BlockSpec(memory_space=pltpu.HBM)] * len(operands)
        + [pl.BlockSpec(memory_space=pltpu.SMEM)],
        out_specs=pl.BlockSpec(memory_space=pltpu.VMEM),
        scratch_shapes=[pltpu.VMEM(x.shape, x.dtype) for x in operands]
        + [
            pltpu.SemaphoreType.DMA((len(operands) - 4,)),
            pltpu.VMEM((shards, pack_rows, TILE), F32),
            pltpu.VMEM((pack_rows, TILE), F32),
            pltpu.VMEM((1, TILE), F32),
            pltpu.VMEM((device_total, 1, TILE), F32),
            pltpu.VMEM((3, 6 * FEATURES, nodes), BF16),
            pltpu.VMEM((clusters, leaves), BF16),
            pltpu.VMEM((2, device_total, nodes), BF16),
            pltpu.VMEM((TILE, TILE), F32),
            pltpu.VMEM((TILE, device_total), F32),
            pltpu.VMEM((source_tiles, 3, 8, nodes), F32),
            pltpu.SemaphoreType.DMA,
            pltpu.SemaphoreType.DMA((shards // 2,)),
            pltpu.SemaphoreType.DMA,
            pltpu.SemaphoreType.DMA,
            pltpu.SemaphoreType.DMA,
            pltpu.SemaphoreType.DMA((groups - 1,)),
        ],
        compiler_params=pltpu.CompilerParams(collective_id=0, has_side_effects=True),
    )(*operands, block_count)
    return leaf_emit + leaf_albedo * gathered


def body(groups, shards, *args):
    leaves, nodes, slots = args[3].shape[0], args[5].shape[1], args[7].shape[1]
    per_shard = (nodes - leaves) // TILE
    source_tiles = shards * per_shard
    dense = (
        nodes // TILE * source_tiles <= TILE
        and TILE % source_tiles == 0
        and source_tiles % 8 == 0
        and nodes % (2 * TILE) == 0
        and leaves % TILE == 0
        and groups > 1
        and nodes % shards == 0
        and nodes // shards <= TILE
        and shards & (shards - 1) == 0
        and shards % 2 == 0
        and groups & (groups - 1) == 0
        and groups * shards <= TILE
        and slots == TILE
    )
    return dense_body(groups, shards, *args) if dense else listed_body(*args)


def solution(mesh):
    in_specs = (
        P(None, "dev"),
        P(None, "dev"),
        P(None, "dev"),
        P("dev"),
        P("dev"),
        P(None, "dev"),
        P(None, "dev"),
        P("grp", "dev"),
        P("grp", "dev"),
        P("grp", "dev"),
    )
    out_specs = P(None, "dev")
    sized = functools.partial(body, mesh.shape["grp"], mesh.shape["dev"])
    return jax.shard_map(sized, mesh=mesh, in_specs=in_specs, out_specs=out_specs, check_vma=False)
```

```python
import functools
import jax
import jax.numpy as jnp
from jax import lax
from jax.experimental import pallas as pl
from jax.experimental.pallas import tpu as pltpu
from jax.sharding import PartitionSpec as P

TILE = 128


batch_slots = 16


def unit_normals(node_angles):
    azimuth = node_angles[0]
    elevation = node_angles[1]
    return jnp.stack(
        [
            jnp.cos(azimuth) * jnp.cos(elevation),
            jnp.sin(azimuth) * jnp.cos(elevation),
            jnp.sin(elevation),
        ]
    )


def tile_irradiance(receivers, sources):
    offsets = [
        sources[axis_id][:, None, :] - receivers[axis_id][:, :, None] for axis_id in range(3)
    ]
    distance_sq = offsets[0] * offsets[0] + offsets[1] * offsets[1] + offsets[2] * offsets[2]
    facing_receiver = (
        receivers[3][:, :, None] * offsets[0]
        + receivers[4][:, :, None] * offsets[1]
        + receivers[5][:, :, None] * offsets[2]
    )
    facing_source = (
        sources[3][:, None, :] * offsets[0]
        + sources[4][:, None, :] * offsets[1]
        + sources[5][:, None, :] * offsets[2]
    )
    source_area = sources[6][:, None, :]
    factor = (
        source_area
        * jnp.maximum(facing_receiver, 0.0)
        * jnp.maximum(-facing_source, 0.0)
        / ((distance_sq + source_area) * (jnp.pi * distance_sq + source_area))
    )
    return jnp.einsum("bij,cbj->bci", factor, sources[7:10], precision=lax.Precision.HIGHEST)


def listed_body(
    leaf_emit,
    leaf_albedo,
    leaf_radiosity,
    leaf_area,
    parent_index,
    node_position,
    node_angles,
    block_receiver,
    block_source,
    block_count,
):
    leaf_count = leaf_area.shape[0]
    node_count = node_position.shape[1]
    cluster_count = node_count - leaf_count
    tile_count = node_count // TILE
    slot_count = block_receiver.shape[1]
    normals = unit_normals(node_angles)
    parent_onehot = (
        parent_index[:, None] == jnp.arange(cluster_count, dtype=jnp.int32)[None, :]
    ).astype(jnp.float32)
    cluster_area = jnp.dot(leaf_area, parent_onehot, precision=lax.Precision.HIGHEST)
    weighted = jnp.dot(
        leaf_radiosity * leaf_area[None, :], parent_onehot, precision=lax.Precision.HIGHEST
    )
    cluster_radiosity = weighted / cluster_area[None, :]
    source_pack = jnp.concatenate(
        [
            node_position[:, leaf_count:],
            normals[:, leaf_count:],
            cluster_area[None, :],
            cluster_radiosity,
        ],
        axis=0,
    )
    receiver_pack = jnp.concatenate([node_position, normals], axis=0)
    linked = lax.all_to_all(receiver_pack, "dev", split_axis=1, concat_axis=1, tiled=True)
    receiver_tiles = linked.reshape(6, tile_count, TILE)
    everything = lax.all_gather(source_pack, "dev", axis=1, tiled=True)
    source_tiles = everything.reshape(10, -1, TILE)
    receiver_ids = block_receiver[0]
    source_ids = block_source[0]
    live_count = block_count[0, 0]
    step_slots = min(batch_slots, slot_count)

    def add_batch(rounds, totals):
        first = rounds * step_slots
        batch_receivers = lax.dynamic_slice_in_dim(receiver_ids, first, step_slots, 0)
        batch_sources = lax.dynamic_slice_in_dim(source_ids, first, step_slots, 0)
        batch_weight = (first + jnp.arange(step_slots, dtype=jnp.int32) < live_count).astype(
            jnp.float32
        )
        receivers = jnp.take(receiver_tiles, batch_receivers, axis=1)
        sources = jnp.take(source_tiles, batch_sources, axis=1)
        contrib = tile_irradiance(receivers, sources) * batch_weight[:, None, None]
        placement = (
            batch_receivers[:, None] == jnp.arange(tile_count, dtype=jnp.int32)[None, :]
        ).astype(jnp.float32)
        return totals + jnp.einsum(
            "bt,bci->cti", placement, contrib, precision=lax.Precision.HIGHEST
        )

    batch_total = (live_count + step_slots - 1) // step_slots
    totals = lax.fori_loop(0, batch_total, add_batch, jnp.zeros((3, tile_count, TILE), jnp.float32))
    partial_value = totals.reshape(3, node_count)
    summed = lax.psum(partial_value, "grp")
    irradiance = lax.all_to_all(summed, "dev", split_axis=1, concat_axis=1, tiled=True)
    pushed = jnp.dot(irradiance[:, leaf_count:], parent_onehot.T, precision=lax.Precision.HIGHEST)
    gathered = irradiance[:, :leaf_count] + pushed
    return leaf_emit + leaf_albedo * gathered


F32 = jnp.float32
BF16 = jnp.bfloat16
MESH = pl.DeviceIdType.MESH
NT_DIMS = (((1,), (1,)), ((), ()))
FEATURES = 8
RELAY_TURN = 4
HELD_PAIRS = 1
ROWS = 64


def split3(values):
    high = values.astype(BF16).astype(F32)
    rest = values - high
    middle = rest.astype(BF16).astype(F32)
    return high, middle, rest - middle


def stack3(values):
    rows = values.shape[0]
    pad = jnp.zeros((16 - 3 * rows, values.shape[1]), F32)
    return jnp.concatenate(list(split3(values)) + [pad], axis=0).astype(BF16)


def unstack3(product, rows):
    return product[0:rows] + product[rows : 2 * rows] + product[2 * rows : 3 * rows]


def flip(k, turn, shards):
    value, bit = 0, 1
    while bit < shards:
        digit = k // bit % 2
        value = value + bit * ((1 - digit) if turn // bit % 2 else digit)
        bit *= 2
    return value


def all_bits(g, pattern, groups, wanted):
    value, bit = 1, 1
    while bit < groups:
        if pattern // bit % 2:
            digit = g // bit % 2
            value = value * (digit if wanted else 1 - digit)
        bit *= 2
    return value


def paired_rows(left, const):
    one, two, three = split3(left)
    row = lax.broadcasted_iota(jnp.int32, left.shape, 0)
    free = (row == 6) | (row == 7)
    plain = [jnp.where(free, 0.0, part) for part in (one, two, three)]
    zero = jnp.zeros_like(left)
    c1, c2, c3 = [zero] * 3 if const is None else split3(jnp.broadcast_to(const, left.shape))
    at6 = row == 6
    with_sum = jnp.where(free, left, one)
    return jnp.concatenate(
        [
            with_sum,
            jnp.where(at6, c1, plain[1]),
            jnp.where(at6, c2, plain[2]),
            with_sum,
            jnp.where(at6, c3, plain[1]),
            with_sum,
        ],
        axis=0,
    ).astype(BF16)


def dense_kernel(groups, shards, *refs):
    operands, count, out, inputs, scratch = refs[:7], refs[7], refs[8], refs[9:16], refs[16:]
    receiver_id, source_id, area, parent, angles, radiosity, position = inputs
    (
        load,
        sources, my_pack, my_hist, hists, right, onehot, place, columns, turned, sums,
        src_send, src_recv, hist_send, hist_recv, pass_send, peer_recv,
    ) = scratch
    g = lax.axis_index("grp")
    k = lax.axis_index("dev")
    device_total = groups * shards
    me = g * shards + k
    leaves = radiosity.shape[1]
    nodes = position.shape[1]
    clusters = nodes - leaves
    per_shard = clusters // TILE
    source_tiles = shards * per_shard
    per_peer = nodes // shards
    chunks = nodes // TILE
    pairs = nodes // (2 * TILE)

    loads = [
        pltpu.make_async_copy(operands[i], inputs[i], load.at[max(i - 4, 0)])
        for i in range(len(inputs))
    ]
    for copy in loads:
        copy.start()

    barrier = pltpu.get_barrier_semaphore()
    group = [flip(g, e, groups) for e in range(groups)]
    drops = [all_bits(g, e, groups, True) for e in range(groups)]
    clear = [all_bits(g, e, groups, False) for e in range(groups)]

    def rows_done(rows, semaphore):
        some = hists.at[pl.ds(0, rows)]
        pltpu.make_async_copy(some, some, semaphore).wait()

    def greet(e, shard):
        pl.semaphore_signal(
            barrier, inc=1, device_id=(group[e], shard), device_id_type=MESH
        )

    def run(first, last, action):
        lax.fori_loop(first, last, lambda shard, _: (action(shard), 0)[1], 0)

    for step in range(1, shards):
        greet(0, flip(k, step, shards))
    for e in reversed(range(1, groups)):
        run(k * (1 - clear[e]), shards, lambda shard: greet(e, shard))

    rows_done(sum(x.size for x in inputs[:5]) // TILE, load.at[0])
    for copy in loads[5:]:
        copy.wait()

    lane = lax.broadcasted_iota(jnp.int32, (1, TILE), 1)
    code = jnp.where(
        lane < count[0, 0], receiver_id[...] * source_tiles + source_id[...], -1
    )
    square = lax.broadcasted_iota(jnp.int32, (TILE, TILE), 0)
    hit = jnp.where(square == code, 1.0, 0.0).astype(BF16)
    counted = lax.dot_general(
        jnp.ones((16, TILE), BF16), hit, NT_DIMS, preferred_element_type=F32
    )
    my_hist[...] = counted[0:1]
    hists[me] = counted[0:1]

    ids = lax.broadcasted_iota(jnp.int32, (clusters, leaves), 0)
    onehot[...] = jnp.where(ids == parent[...], 1.0, 0.0).astype(BF16)
    area_row = area[...]
    stacked = stack3(jnp.concatenate([area_row, radiosity[...] * area_row], axis=0))
    cluster = unstack3(
        lax.dot_general(stacked, onehot[...], NT_DIMS, preferred_element_type=F32), 4
    )
    cosines = jnp.cos(angles[...])
    sines = jnp.sin(angles[...])
    normals = jnp.concatenate(
        [cosines[0:1] * cosines[1:2], sines[0:1] * cosines[1:2], sines[1:2]], axis=0
    )
    first_band = cluster[1:2] * (1.0 / jnp.pi)
    facing = normals[:, leaves:] * first_band
    ratios = cluster[2:4] / cluster[1:2]
    for half in range(per_shard):
        here = slice(half * TILE, (half + 1) * TILE)
        there = slice(leaves + half * TILE, leaves + (half + 1) * TILE)
        my_pack[8 * half : 8 * half + 8, :] = jnp.concatenate(
            [position[:, there], facing[:, here], cluster[0:1, here], ratios[0:1, here]], axis=0
        )
        my_pack[8 * per_shard + half : 8 * per_shard + half + 1, :] = ratios[1:2, here]

    drop_total = sum(drops[1:], 1)
    pl.semaphore_wait(barrier, groups - 1 + groups * k + (shards - 1 - k) * drop_total)

    def hist_copy(e, shard):
        return pltpu.make_async_remote_copy(
            src_ref=my_hist,
            dst_ref=hists.at[me],
            send_sem=hist_send,
            recv_sem=hist_recv,
            device_id=(group[e], shard),
            device_id_type=MESH,
        )

    def peer_copy(e):
        return pltpu.make_async_remote_copy(
            src_ref=my_hist,
            dst_ref=hists.at[me],
            send_sem=hist_send,
            recv_sem=peer_recv.at[e - 1],
            device_id=(group[e], k),
            device_id_type=MESH,
        )

    def passed_copy(e, shard):
        return pltpu.make_async_remote_copy(
            src_ref=hists.at[group[e] * shards + k],
            dst_ref=hists.at[group[e] * shards + k],
            send_sem=pass_send,
            recv_sem=hist_recv,
            device_id=(g, shard),
            device_id_type=MESH,
        )

    def source_copy(shard):
        return pltpu.make_async_remote_copy(
            src_ref=my_pack,
            dst_ref=sources.at[k],
            send_sem=src_send,
            recv_sem=src_recv.at[k // 2],
            device_id=(g, shard),
            device_id_type=MESH,
        )

    run(0, k, lambda shard: hist_copy(groups - 1, shard).start())
    run(0, k, lambda shard: source_copy(shard).start())
    run(k + 1, shards, lambda shard: source_copy(shard).start())
    for e in reversed(range(groups - 1)):
        run(0, k, lambda shard: hist_copy(e, shard).start())
    for e in range(1, groups):
        peer_copy(e).start()
    for e in range(groups):

        @pl.when(drops[e] == 1)
        def _():
            run(k + 1, shards, lambda shard: hist_copy(e, shard).start())

    middle = jnp.sum(position[...], axis=1, keepdims=True) * (1.0 / nodes)
    centred = position[...] - middle
    ones = jnp.ones((1, nodes), F32)
    none = jnp.zeros((1, nodes), F32)
    three = jnp.zeros((3, nodes), F32)
    offset = -jnp.sum(normals * centred, axis=0, keepdims=True)
    norm = jnp.sum(centred * centred, axis=0, keepdims=True)
    for which, rows in enumerate(
        (
            paired_rows(jnp.concatenate([normals, three, none, none], axis=0), offset),
            paired_rows(jnp.concatenate([three, centred, -ones, none], axis=0), None),
            paired_rows(jnp.concatenate([-2.0 * centred, three, none, ones], axis=0), norm),
        )
    ):
        right[which] = rows

    node = lax.broadcasted_iota(jnp.int32, (1, nodes), 1)
    link = jnp.zeros((1, nodes), jnp.int32)
    for j in range(1, shards):
        link += jnp.where(node >= j * per_peer, 1, 0)
    spot = k * per_peer + node - link * per_peer
    low_tile = k * per_peer // TILE
    high_tile = (k * per_peer + per_peer - 1) // TILE
    upper = spot >= (low_tile + 1) * TILE
    owner_row = lax.broadcasted_iota(jnp.int32, (device_total, nodes), 0) % shards
    hits = owner_row == link
    place[0] = jnp.where(hits & ~upper, 1.0, 0.0).astype(BF16)
    place[1] = jnp.where(hits & upper, 1.0, 0.0).astype(BF16)

    row8 = lax.broadcasted_iota(jnp.int32, (8, TILE), 0)
    centre8 = jnp.concatenate([middle, jnp.zeros((5, 1), F32)], axis=0)

    def prepare(pack, half, tile):
        values = pack[8 * half : 8 * half + 8, :]
        ratio = pack[8 * per_shard + half : 8 * per_shard + half + 1, :]
        area_here = values[6:7]
        shifted = values - centre8
        spots, aims = shifted[0:3], shifted[3:6]
        along = jnp.sum(spots * aims, axis=0, keepdims=True)
        reach = jnp.sum(spots * spots, axis=0, keepdims=True) + area_here
        one, two, low = split3(jnp.concatenate([spots, aims, along, reach], axis=0))
        left = jnp.concatenate(
            [
                one,
                jnp.where(row8 == 6, 1.0, one),
                jnp.where(row8 == 6, 1.0, one),
                two,
                jnp.where(row8 == 6, 1.0, two),
                low,
            ],
            axis=0,
        )
        extra = jnp.concatenate(
            [values[7:8], ratio, area_here * ((jnp.pi - 1.0) / jnp.pi), jnp.zeros((5, TILE), F32)],
            axis=0,
        )
        features = jnp.transpose(left).astype(BF16)
        column = jnp.transpose(extra)
        second, third, less = [
            jnp.broadcast_to(column[:, i : i + 1], (TILE, TILE)) for i in range(3)
        ]
        return features, second, third, less, tile

    def products(features, pair):
        wide = slice(pair * 2 * TILE, (pair + 1) * 2 * TILE)
        return [
            [
                jnp.dot(
                    features[first : first + ROWS], right[which, :, wide],
                    preferred_element_type=F32,
                )
                for which in range(3)
            ]
            for first in range(0, TILE, ROWS)
        ]

    def finish(parts, pair, second, third, less, tile):
        totals = [[None] * 3, [None] * 3]
        for first, (toward, facing, span) in zip(range(0, TILE, ROWS), parts):
            some = slice(first, first + ROWS)
            for side in range(2):
                lanes = slice(side * TILE, (side + 1) * TILE)
                u = span[:, lanes]
                form = (
                    jnp.maximum(toward[:, lanes], 0.0)
                    * jnp.maximum(facing[:, lanes], 0.0)
                    / (u * (u - less[some]))
                )
                for c, scaled in enumerate((form, form * second[some], form * third[some])):
                    part = jnp.sum(scaled.reshape(ROWS // 8, 8, TILE), axis=0)
                    old = totals[side][c]
                    totals[side][c] = part if old is None else old + part
        for side in range(2):
            first = pair * 2 * TILE + side * TILE
            for c in range(3):
                sums[tile, c, :, first : first + TILE] = totals[side][c]

    def settle():
        everything = sources.at[pl.ds(0, shards - 1)]
        pltpu.make_async_copy(everything, everything, src_send).wait()
        levels = [1]
        while levels[-1] < groups:
            levels.append(2 * levels[-1])
        for shard in range(shards):

            @pl.when(k == shard)
            def _():
                for level in levels:
                    later = shards - 1 - shard
                    rows = groups - 1 + groups * shard + later * level
                    passed = later * (groups - groups // level)

                    @pl.when(drop_total == level)
                    def _():
                        rows_done(rows, hist_send)
                        if passed:
                            rows_done(passed, pass_send)

    def peer_arrival(e):
        pltpu.make_async_remote_copy(
            src_ref=my_hist,
            dst_ref=hists.at[group[e] * shards + k],
            send_sem=hist_send,
            recv_sem=peer_recv.at[e - 1],
            device_id=(group[e], k),
            device_id_type=MESH,
        ).wait_recv()

    held = []
    for first in range(0, shards, 2):
        if first == RELAY_TURN:
            for e in range(1, groups):

                @pl.when(clear[e] == 0)
                def _():
                    peer_arrival(e)
                    run(k + 1, shards, lambda shard: passed_copy(e, shard).start())

        if first == shards - 2:
            settle()
        owners = [flip(k, first, shards), flip(k, first + 1, shards)]
        if first:
            both = sources.at[pl.ds(owners[0] // 2 * 2, 2)]
        else:
            both = sources.at[owners[1]]
        pltpu.make_async_copy(both, both, src_recv.at[owners[0] // 2]).wait()
        packs = [(sources.at[owner], owner) for owner in owners]
        if not first:
            packs[0] = (my_pack, k)
        ready = [
            prepare(pack, half, owner * per_shard + half)
            for pack, owner in packs
            for half in range(per_shard)
        ]
        for work in held:
            finish(*work)
        held = []
        for number, (features, *rest) in enumerate(ready):
            for pair in range(pairs):
                work = (products(features, pair), pair, *rest)
                if number == len(ready) - 1 and pair >= pairs - HELD_PAIRS:
                    held.append(work)
                else:
                    finish(*work)

    for e in range(1, groups):

        @pl.when(clear[e] == 1)
        def _():
            peer_arrival(e)

    distant = hists.at[pl.ds(0, groups * (shards - 1))]
    pltpu.make_async_copy(distant, distant, hist_recv).wait()
    table = hists[...].reshape(device_total, TILE)
    turned[...] = jnp.transpose(table)
    weight = jnp.zeros((source_tiles, nodes), F32)
    for which, tile in enumerate((low_tile, high_tile)):
        rows = turned[pl.ds(pl.multiple_of(tile * source_tiles, 8), source_tiles), :]
        weight += jnp.dot(rows.astype(BF16), place[which], preferred_element_type=F32)
    for work in held:
        finish(*work)

    chunk_rows = []
    for chunk in range(chunks):
        lanes = slice(chunk * TILE, (chunk + 1) * TILE)
        totals = [None] * 3
        for tile in range(source_tiles):
            scale = jnp.broadcast_to(weight[tile : tile + 1, lanes], (8, TILE))
            for c in range(3):
                part = scale * sums[tile, c, :, lanes]
                totals[c] = part if totals[c] is None else totals[c] + part
        chunk_rows.append(
            jnp.concatenate([jnp.sum(x, axis=0, keepdims=True) for x in totals], axis=0)
        )
    irradiance = jnp.concatenate(chunk_rows, axis=1)
    pushed = unstack3(
        jnp.dot(stack3(irradiance[:, leaves:]), onehot[...], preferred_element_type=F32), 3
    )
    out[...] = irradiance[:, :leaves] + pushed


def dense_body(
    groups, shards, leaf_emit, leaf_albedo, leaf_radiosity, leaf_area, parent_index,
    node_position, node_angles, block_receiver, block_source, block_count,
):
    leaves = leaf_area.shape[0]
    nodes = node_position.shape[1]
    clusters = nodes - leaves
    per_shard = clusters // TILE
    source_tiles = shards * per_shard
    device_total = groups * shards
    operands = (
        block_receiver, block_source, leaf_area[None, :], parent_index[None, :], node_angles,
        leaf_radiosity, node_position,
    )
    pack_rows = 9 * per_shard
    gathered = pl.pallas_call(
        functools.partial(dense_kernel, groups, shards),
        out_shape=pltpu.VMEM((3, leaves), F32),
        in_specs=[pl.BlockSpec(memory_space=pltpu.HBM)] * len(operands)
        + [pl.BlockSpec(memory_space=pltpu.SMEM)],
        out_specs=pl.BlockSpec(memory_space=pltpu.VMEM),
        scratch_shapes=[pltpu.VMEM(x.shape, x.dtype) for x in operands]
        + [
            pltpu.SemaphoreType.DMA((len(operands) - 4,)),
            pltpu.VMEM((shards, pack_rows, TILE), F32),
            pltpu.VMEM((pack_rows, TILE), F32),
            pltpu.VMEM((1, TILE), F32),
            pltpu.VMEM((device_total, 1, TILE), F32),
            pltpu.VMEM((3, 6 * FEATURES, nodes), BF16),
            pltpu.VMEM((clusters, leaves), BF16),
            pltpu.VMEM((2, device_total, nodes), BF16),
            pltpu.VMEM((TILE, TILE), F32),
            pltpu.VMEM((TILE, device_total), F32),
            pltpu.VMEM((source_tiles, 3, 8, nodes), F32),
            pltpu.SemaphoreType.DMA,
            pltpu.SemaphoreType.DMA((shards // 2,)),
            pltpu.SemaphoreType.DMA,
            pltpu.SemaphoreType.DMA,
            pltpu.SemaphoreType.DMA,
            pltpu.SemaphoreType.DMA((groups - 1,)),
        ],
        compiler_params=pltpu.CompilerParams(collective_id=0, has_side_effects=True),
    )(*operands, block_count)
    return leaf_emit + leaf_albedo * gathered


def body(groups, shards, *args):
    leaves, nodes, slots = args[3].shape[0], args[5].shape[1], args[7].shape[1]
    per_shard = (nodes - leaves) // TILE
    source_tiles = shards * per_shard
    dense = (
        nodes // TILE * source_tiles <= TILE
        and TILE % source_tiles == 0
        and source_tiles % 8 == 0
        and nodes % (2 * TILE) == 0
        and leaves % TILE == 0
        and groups > 1
        and nodes % shards == 0
        and nodes // shards <= TILE
        and shards & (shards - 1) == 0
        and shards % 2 == 0
        and groups & (groups - 1) == 0
        and groups * shards <= TILE
        and slots == TILE
    )
    return dense_body(groups, shards, *args) if dense else listed_body(*args)


def solution(mesh):
    in_specs = (
        P(None, "dev"),
        P(None, "dev"),
        P(None, "dev"),
        P("dev"),
        P("dev"),
        P(None, "dev"),
        P(None, "dev"),
        P("grp", "dev"),
        P("grp", "dev"),
        P("grp", "dev"),
    )
    out_specs = P(None, "dev")
    sized = functools.partial(body, mesh.shape["grp"], mesh.shape["dev"])
    return jax.shard_map(sized, mesh=mesh, in_specs=in_specs, out_specs=out_specs, check_vma=False)
```
